128 devices in a mesh: pts: 32 (over x, y, core), cam: 4 (over z).
Axes of the slice: x: 4, y: 4, z: 4, core: 2. Of those that a mesh axis runs over, the one named last changes fastest.
Arguments:
- cameras: float32 [9, 16384], P(None, ('pts', 'cam')), may hold values from -0.5 to 2
- increment: float32 [9, 16384], P(None, ('pts', 'cam')), may hold values from -0.3 to 0.3
- points: float32 [3, 2097152], P(None, 'pts'), may hold values from -6 to 2
- point_gradient: float32 [3, 2097152], P(None, 'pts'), may hold values from -1.8 to 1.8
- point_inverse: float32 [9, 2097152], P(None, 'pts'), may hold values from -0.35 to 1.6, as said below
- cam_jacobian: bfloat16 [18, 33554432], P(None, ('pts', 'cam')), may hold values from -3 to 3
- point_jacobian: bfloat16 [6, 33554432], P(None, ('pts', 'cam')), may hold values from -3 to 3
- observed: float32 [2, 33554432], P(None, ('pts', 'cam')), may hold values from -10 to 10
- tile_block: int32 [131072], P(('pts', 'cam')), may hold values from 0 to 127
- tile_points: int32 [131072], P(('pts', 'cam')), may hold values from 0 to 255
- obs_camera: int32 [33554432], P(('pts', 'cam')), may hold values from 0 to 127
- obs_point: int32 [33554432], P(('pts', 'cam')), may hold values from 0 to 255
- accept: int32 [], replicated, may hold values from 0 to 1073741823
Outputs:
- residual: float32 [2, 33554432], P(None, ('pts', 'cam'))
- trial_cost: float32 [], replicated
- accepted_points: float32 [3, 2097152], P(None, 'pts')
- accepted_cameras: float32 [9, 16384], P(None, ('pts', 'cam'))
The draws below stay inside these ranges and needn't reach their ends.
Inputs may be any that keep to these rules, and one draw needn't show every extreme that they name: `tile_block`: the block of 128 cameras that all 256 observations of a tile look at. `tile_points`: the block of 256 points of its point group that all 256 observations of a tile look at. `obs_camera`: an observation's camera within its tile's block. `obs_point`: an observation's point within its tile's point block. `accept`: an odd word accepts the step, an even one keeps the old parameters. `point_inverse`: each 3 x 3 block is symmetric with a dominant positive diagonal.
All inputs are finite; a program needn't handle non-finite values.
Results may differ from the reference program's by a relative error of at most 0.0003.
Values sent between devices are 32-bit elements; how exact they have to be, the bound alone decides.
A program may use at most 192 MiB of HBM per device.

```python
import math
import jax
import jax.numpy as jnp
from jax import lax

CB = 128
PB = 256
TILE = 256
PTS_DEV = 65536
OBS_GROUP = 1048576
NOBS = 33554432
NPTS = 2097152
CAMS = 16384
N_PTS = 32


def draw_cameras(key, part):
    keys = jax.random.split(jax.random.fold_in(key, 11), 4)
    rotation = jax.random.uniform(keys[0], (3, CAMS), jnp.float32, -0.3, 0.3)
    shifted = jnp.clip(0.2 * jax.random.normal(keys[1], (3, CAMS), jnp.float32), -0.5, 0.5)
    focal = jax.random.uniform(keys[2], (1, CAMS), jnp.float32, 0.6, 1.4)
    radial = jax.random.uniform(keys[3], (2, CAMS), jnp.float32, -1.0, 1.0) * jnp.array([[0.05], [0.005]], jnp.float32)
    return jnp.concatenate([rotation, shifted, focal, radial], axis=0)


def draw_increment(key, part):
    keys = jax.random.split(jax.random.fold_in(key, 17), 1)
    scales = jnp.array([0.05, 0.05, 0.05, 0.1, 0.1, 0.1, 0.05, 0.01, 0.002], jnp.float32).reshape(9, 1)
    values = jnp.clip(jax.random.normal(keys[0], (9, CAMS), jnp.float32), -3.0, 3.0)
    return values * scales


def draw_points(key, part):
    keys = jax.random.split(jax.random.fold_in(key, 19), 2)
    planar = jax.random.uniform(keys[0], (2, NPTS), jnp.float32, -2.0, 2.0)
    height = jax.random.uniform(keys[1], (1, NPTS), jnp.float32, -6.0, -0.8)
    return jnp.concatenate([planar, height], axis=0)


def draw_point_inverse(key, part):
    keys = jax.random.split(jax.random.fold_in(key, 23), 2)
    diagonal = jax.random.uniform(keys[0], (3, NPTS), jnp.float32, 0.8, 1.6)
    offdiag = jax.random.uniform(keys[1], (3, NPTS), jnp.float32, -0.35, 0.35)
    return jnp.stack([diagonal[0], offdiag[0], offdiag[1], offdiag[0], diagonal[1], offdiag[2], offdiag[1], offdiag[2], diagonal[2]])


def draw_observed(key, part):
    keys = jax.random.split(jax.random.fold_in(key, 29), 2)
    position = lax_free_iota()
    level = 0.5 * jnp.exp(math.log(3.0) * position / NOBS)
    spread = jnp.exp(jax.random.uniform(keys[1], (2, NOBS), jnp.float32, math.log(0.5), math.log(2.0)))
    values = jnp.clip(jax.random.normal(keys[0], (2, NOBS), jnp.float32), -3.0, 3.0)
    return values * level * spread


def lax_free_iota():
    return jnp.arange(NOBS, dtype=jnp.float32).reshape(1, NOBS)


def plant(entries, key, smallest, high):
    shape = entries.shape
    place = [jax.random.randint(jax.random.fold_in(key, axis), (), 0, shape[axis]) for axis in range(len(shape))]
    entries = entries.at[tuple(place)].set(smallest)
    longest = shape.index(max(shape))
    place[longest] = (place[longest] + 1) % shape[longest]
    return entries.at[tuple(place)].set(high)


def block_scale(own_key, extent, cuts, low, high):
    factor_of, own = 1.0, jax.random.fold_in(own_key, 6)
    for dim, blocks in cuts:
        steps = jnp.exp(jax.random.uniform(jax.random.fold_in(own, dim), (blocks,), jnp.float32, low / len(cuts), high / len(cuts)))
        factor_of = factor_of * jnp.repeat(steps, extent[dim] // blocks).reshape([-1 if axis == dim else 1 for axis in range(len(extent))])
    return factor_of


def centred(rng, shape, width, most, pieces=(), kind=jnp.bfloat16):
    loudness = block_scale(rng, shape, pieces, -0.22, 0.18) if pieces else 1.0
    values = jax.random.normal(rng, shape, jnp.float32) * width * loudness
    return jnp.minimum(jnp.maximum(values, -most), most).astype(kind)


def setup_inputs(seed: int = 0) -> dict:
    arg_keys = jax.random.split(jax.random.key(seed), 14)
    return {
        "cameras": draw_cameras(jax.random.fold_in(arg_keys[13], 71), 0),
        "increment": draw_increment(jax.random.fold_in(arg_keys[13], 71), 0),
        "points": draw_points(jax.random.fold_in(arg_keys[13], 71), 0),
        "point_gradient": centred(arg_keys[3], (3, NPTS), 0.3, 1.8, ((1, 32),), jnp.float32),
        "point_inverse": draw_point_inverse(jax.random.fold_in(arg_keys[13], 71), 0),
        "cam_jacobian": centred(arg_keys[5], (18, NOBS), 0.5, 3.0, ((1, 128),)),
        "point_jacobian": centred(arg_keys[6], (6, NOBS), 0.5, 3.0, ((1, 128),)),
        "observed": draw_observed(jax.random.fold_in(arg_keys[13], 71), 0),
        "tile_block": plant(jax.random.randint(arg_keys[8], (NOBS // TILE,), 0, CAMS // CB), jax.random.fold_in(arg_keys[8], 1), 0, (CAMS // CB) - 1).astype(jnp.int32),
        "tile_points": plant(jax.random.randint(arg_keys[9], (NOBS // TILE,), 0, PTS_DEV // PB), jax.random.fold_in(arg_keys[9], 1), 0, (PTS_DEV // PB) - 1).astype(jnp.int32),
        "obs_camera": plant(jax.random.randint(arg_keys[10], (NOBS,), 0, CB), jax.random.fold_in(arg_keys[10], 1), 0, CB - 1).astype(jnp.int32),
        "obs_point": plant(jax.random.randint(arg_keys[11], (NOBS,), 0, PB), jax.random.fold_in(arg_keys[11], 1), 0, PB - 1).astype(jnp.int32),
        "accept": jax.random.randint(arg_keys[12], (), 0, 1073741824).astype(jnp.int32),
    }


def rotate_point(angles, coords):
    angle_size = jnp.sqrt(lax.optimization_barrier(jnp.sum(angles * angles, axis=0)))
    cosine = jnp.cos(angle_size)
    sine_ratio = jnp.sinc(angle_size / math.pi)
    cosine_ratio = 0.5 * jnp.square(jnp.sinc(angle_size / (2.0 * math.pi)))
    crossed = jnp.stack([angles[1] * coords[2] - angles[2] * coords[1], angles[2] * coords[0] - angles[0] * coords[2], angles[0] * coords[1] - angles[1] * coords[0]])
    inner_part = lax.optimization_barrier(jnp.sum(angles * coords, axis=0))
    return cosine * coords + sine_ratio * crossed + cosine_ratio * inner_part * angles

def project(camera, coords):
    placed = rotate_point(camera[0:3], coords) + camera[3:6]
    depth_clip = jnp.maximum(-placed[2], 1.0)
    planar = placed[0:2] / depth_clip
    radius = lax.optimization_barrier(jnp.sum(planar * planar, axis=0))
    factor = camera[6] * (1.0 + camera[7] * radius + camera[8] * radius * radius)
    return factor * planar

def couple(cam_rows, point_rows, cam_steps):
    cam_rows = cam_rows.astype(jnp.float32)
    point_rows = point_rows.astype(jnp.float32)
    first_row = lax.optimization_barrier(jnp.sum(cam_rows[0:9] * cam_steps, axis=0))
    second_row = lax.optimization_barrier(jnp.sum(cam_rows[9:18] * cam_steps, axis=0))
    return point_rows[0:3] * first_row + point_rows[3:6] * second_row

def solve_points(inverse, gradient, reduced):
    residue = gradient - reduced
    return jnp.stack([inverse[3 * target] * residue[0] + inverse[3 * target + 1] * residue[1] + inverse[3 * target + 2] * residue[2] for target in range(3)])

def reference(cameras, increment, points, point_gradient, point_inverse, cam_jacobian, point_jacobian, observed, tile_block, tile_points, obs_camera, obs_point, accept):
    trial_cameras = cameras + increment
    group_tiles = OBS_GROUP // TILE

    def segment_rows(values, owners):
        return jax.ops.segment_sum(values, owners, num_segments=PTS_DEV)

    def one_group(group_id):
        obs_start = (group_id * OBS_GROUP).astype(jnp.int32)
        tile_start = (group_id * group_tiles).astype(jnp.int32)
        chosen = lax.dynamic_slice_in_dim(tile_block, tile_start, group_tiles, 0)
        chosen_points = lax.dynamic_slice_in_dim(tile_points, tile_start, group_tiles, 0)
        cam_local = lax.dynamic_slice_in_dim(obs_camera, obs_start, OBS_GROUP, 0)
        cam_which = (jnp.repeat(chosen, TILE) * CB + cam_local).astype(jnp.int32)
        step_rows = jnp.take(increment, cam_which, axis=1)
        trial_rows = jnp.take(trial_cameras, cam_which, axis=1)
        coupling = couple(lax.dynamic_slice_in_dim(cam_jacobian, obs_start, OBS_GROUP, 1), lax.dynamic_slice_in_dim(point_jacobian, obs_start, OBS_GROUP, 1), step_rows)
        point_local = lax.dynamic_slice_in_dim(obs_point, obs_start, OBS_GROUP, 0)
        owners = (jnp.repeat(chosen_points, TILE) * PB + point_local).astype(jnp.int32)
        reduced = jax.vmap(segment_rows, in_axes=(0, None))(coupling, owners)
        point_start = (group_id * PTS_DEV).astype(jnp.int32)
        own_points = lax.dynamic_slice_in_dim(points, point_start, PTS_DEV, 1)
        point_step = solve_points(lax.dynamic_slice_in_dim(point_inverse, point_start, PTS_DEV, 1), lax.dynamic_slice_in_dim(point_gradient, point_start, PTS_DEV, 1), reduced)
        seen_points = jnp.take(own_points + point_step, owners, axis=1)
        residual = project(trial_rows, seen_points) - lax.dynamic_slice_in_dim(observed, obs_start, OBS_GROUP, 1)
        return (residual, point_step, jnp.sum(residual * residual))
    residuals, point_steps, partials = lax.map(one_group, jnp.arange(N_PTS, dtype=jnp.int32))
    residual = jnp.transpose(residuals, (1, 0, 2)).reshape(2, NOBS)
    point_step = jnp.transpose(point_steps, (1, 0, 2)).reshape(3, NPTS)
    trial_cost = jnp.sum(partials) / (2.0 * NOBS)
    accepted_flag = jnp.remainder(accept, 2).astype(jnp.float32)
    return (residual, trial_cost, points + accepted_flag * point_step, cameras + accepted_flag * increment)
```

```python
import functools, math
import jax, jax.numpy as jnp
from jax import lax
from jax.experimental import pallas as pl
from jax.experimental.pallas import tpu as pltpu
from jax.sharding import Mesh
from jax.sharding import PartitionSpec as P

CB=128; PB=256; TILE=256
F32=jnp.float32
GROUP=1024
TPG=GROUP//TILE

def lane_gather(table, index):
    return lax.gather(table, index[..., None],
        lax.GatherDimensionNumbers(offset_dims=(), collapsed_slice_dims=(1,), start_index_map=(1,),
            operand_batching_dims=(0,), start_indices_batching_dims=(0,)),
        slice_sizes=(1,1), mode=lax.GatherScatterMode.PROMISE_IN_BOUNDS)

def tile_rows(rows, row_id):
    a,b,c,d = rows
    return jnp.where(row_id<4, jnp.where(row_id<2,a,b), jnp.where(row_id<6,c,d))

def spread(ref, first):
    return ref[pl.ds(first, 8, stride=0), :]

PH=8; PL=32

def reduce_body(chunk, blocks_n, tb, tp, inc_ref, cj_ref, pj_ref, oc_ref, op_ref, out_ref, acc, jscr, pscr, wscr):
    step = pl.program_id(0)
    groups = chunk//GROUP
    row_id = lax.broadcasted_iota(jnp.int32,(8,128),0)
    @pl.when(step==0)
    def _():
        def zero(i,_):
            acc[pl.ds(pl.multiple_of(i*64,64),64),:] = jnp.zeros((64,PL),F32)
            return 0
        lax.fori_loop(0, blocks_n, zero, 0)
        wscr[...] = jnp.zeros_like(wscr)
    def couple(g, slot):
        base = step*(chunk//TILE) + g*TPG
        cams = [tb[base+i]*9 for i in range(TPG)]
        cam = oc_ref[pl.ds(pl.multiple_of(g*8,8),8),:]
        for j in range(8):
            at = pl.ds(pl.multiple_of(g*GROUP+j*128,128),128)
            jscr[slot, j*24:j*24+18,:] = cj_ref[:,at].astype(F32)
            pscr[slot, j*8:j*8+6,:] = pj_ref[:,at].astype(F32)
        first=second=None
        for m in range(9):
            t = tile_rows([spread(inc_ref, c+m) for c in cams], row_id)
            v = lane_gather(t, cam)
            a = jscr[slot, pl.ds(m,8,stride=24),:]*v
            b = jscr[slot, pl.ds(9+m,8,stride=24),:]*v
            first = a if first is None else first+a
            second = b if second is None else second+b
        for n in range(3):
            v = pscr[slot, pl.ds(n,8,stride=8),:]*first + pscr[slot, pl.ds(3+n,8,stride=8),:]*second
            hi = v.astype(jnp.bfloat16).astype(F32)
            wscr[slot, pl.ds(n,8,stride=8),:] = hi
            wscr[slot, pl.ds(3+n,8,stride=8),:] = v-hi
    def scatter(g, slot):
        base = step*(chunk//TILE) + g*TPG
        for t in range(TPG):
            lhs=[]; rhs=[]
            for h in range(2):
                s=2*t+h
                w = wscr[slot, s*8:s*8+8,:]
                ids = op_ref[pl.ds(g*8+s,8,stride=0),:]
                hi = lax.shift_right_logical(ids,5)
                lo = ids & 31
                lhs.append(jnp.concatenate([jnp.where(hi==k,w,0.0) for k in range(PH)],axis=0).astype(jnp.bfloat16))
                rhs.append(jnp.concatenate([jnp.where(lo-8*k==row_id,1.0,0.0) for k in range(PL//8)],axis=0).astype(jnp.bfloat16))
            L=jnp.concatenate(lhs,axis=1); R=jnp.concatenate(rhs,axis=1)
            r = lax.dot_general(L,R,(((1,),(1,)),((),())),preferred_element_type=F32)
            at = pl.ds(pl.multiple_of(tp[base+t]*64,64),64)
            acc[at,:] += r
    UN=2
    def body(i,_):
        for u in range(UN):
            couple(i*UN+u, u)
            scatter(i*UN+u, u)
        return 0
    lax.fori_loop(0, groups//UN, body, 0)
    @pl.when(step==pl.num_programs(0)-1)
    def _():
        def flush(i,_):
            for h in range(2):
                parts=[]
                for k in range(4):
                    x = acc[pl.ds(pl.multiple_of(i*64+h*32+k*8,8),8),:]
                    parts.append(x)
                x=jnp.concatenate(parts,axis=1)
                s = x[0:3,:]+x[3:6,:]
                out_ref[:, pl.ds(pl.multiple_of(i*PB+h*128,128),128)] = s
            return 0
        lax.fori_loop(0, blocks_n, flush, 0)

def reduce_points(inc, cj, pj, oc, op, tb, tp, npts, chunk=8192):
    n=cj.shape[1]
    blocks_n=npts//PB
    return pl.pallas_call(
        functools.partial(reduce_body, chunk, blocks_n),
        out_shape=jax.ShapeDtypeStruct((3,npts),F32),
        grid_spec=pltpu.PrefetchScalarGridSpec(
            num_scalar_prefetch=2, grid=(n//chunk,),
            in_specs=[
                pl.BlockSpec(inc.shape, lambda i,*_:(0,0)),
                pl.BlockSpec((18,chunk), lambda i,*_:(0,i)),
                pl.BlockSpec((6,chunk), lambda i,*_:(0,i)),
                pl.BlockSpec((chunk//128,128), lambda i,*_:(i,0)),
                pl.BlockSpec((chunk//128,128), lambda i,*_:(i,0)),
            ],
            out_specs=pl.BlockSpec((3,npts), lambda i,*_:(0,0)),
            scratch_shapes=[pltpu.VMEM((blocks_n*64,PL),F32), pltpu.VMEM((2,192,128),F32), pltpu.VMEM((2,64,128),F32), pltpu.VMEM((2,64,128),F32)],
        ),
        compiler_params=pltpu.CompilerParams(dimension_semantics=("arbitrary",), vmem_limit_bytes=48*1024*1024),
        name="reduce_points",
    )(tb,tp,inc,cj,pj,oc,op)

CT=10
def project_body(chunk, tb, tp, cam_ref, pts_ref, oc_ref, op_ref, ob_ref, res_ref, cost_ref):
    step=pl.program_id(0)
    groups=chunk//GROUP
    row_id=lax.broadcasted_iota(jnp.int32,(8,128),0)
    @pl.when(step==0)
    def _():
        cost_ref[...]=jnp.zeros_like(cost_ref)
    def one(g):
        base=step*(chunk//TILE)+g*TPG
        cams=[tb[base+i]*CT for i in range(TPG)]
        pts=[tp[base+i]*8 for i in range(TPG)]
        at8=pl.ds(pl.multiple_of(g*8,8),8)
        cam=oc_ref[at8,:]; pid=op_ref[at8,:]
        upper=pid>=128; plow=pid&127
        def look(r): return lane_gather(tile_rows([spread(cam_ref,c+r) for c in cams],row_id),cam)
        def lookp(r):
            a=lane_gather(tile_rows([spread(pts_ref,p+r) for p in pts],row_id),plow)
            b=lane_gather(tile_rows([spread(pts_ref,p+4+r) for p in pts],row_id),plow)
            return jnp.where(upper,b,a)
        x,y,z=lookp(0),lookp(1),lookp(2)
        vx,vy,vz,r,t0,t1,t2,f0,f1,f2=[look(i) for i in range(CT)]
        ax=vy*z-vz*y; ay=vz*x-vx*z; az=vx*y-vy*x
        px=x+r*ax+(vy*az-vz*ay)+t0
        py=y+r*ay+(vz*ax-vx*az)+t1
        pz=z+r*az+(vx*ay-vy*ax)+t2
        inv=1.0/jnp.maximum(-pz,1.0)
        u=px*inv; v=py*inv
        q=u*u+v*v
        fac=f0+q*(f1+q*f2)
        o0=pl.ds(g*16,8,stride=2); o1=pl.ds(g*16+1,8,stride=2)
        ru=fac*u-ob_ref[o0,:]; rv=fac*v-ob_ref[o1,:]
        res_ref[o0,:]=ru; res_ref[o1,:]=rv
        return ru*ru+rv*rv
    UN=2
    def body(i,c):
        for u in range(UN): c=c+one(i*UN+u)
        return c
    cost_ref[...]+=lax.fori_loop(0,groups//UN,body,jnp.zeros((8,128),F32))

def project_points(cam, pts, oc, op, ob, tb, tp, chunk=8192):
    n=oc.shape[0]*128
    return pl.pallas_call(
        functools.partial(project_body, chunk),
        out_shape=(jax.ShapeDtypeStruct((n//64,128),F32), jax.ShapeDtypeStruct((8,128),F32)),
        grid_spec=pltpu.PrefetchScalarGridSpec(
            num_scalar_prefetch=2, grid=(n//chunk,),
            in_specs=[
                pl.BlockSpec(cam.shape, lambda i,*_:(0,0)),
                pl.BlockSpec(pts.shape, lambda i,*_:(0,0)),
                pl.BlockSpec((chunk//128,128), lambda i,*_:(i,0)),
                pl.BlockSpec((chunk//128,128), lambda i,*_:(i,0)),
                pl.BlockSpec((chunk//64,128), lambda i,*_:(i,0)),
            ],
            out_specs=(pl.BlockSpec((chunk//64,128), lambda i,*_:(i,0)), pl.BlockSpec((8,128), lambda i,*_:(0,0))),
        ),
        compiler_params=pltpu.CompilerParams(dimension_semantics=("arbitrary",), vmem_limit_bytes=32*1024*1024),
        name="project_points",
    )(tb,tp,cam,pts,oc,op,ob)


CAM = "cam"
PTS = ("pts_0", "pts_1", "pts_2")
PTS_CAM = PTS + (CAM,)
RT2 = math.sqrt(2.0)


def camera_rows(trial):
    w = trial[0:3]
    half = 0.5 * jnp.sqrt(jnp.sum(w * w, axis=0, keepdims=True))
    v = (0.5 * RT2) * jnp.sinc(half / math.pi) * w
    r = RT2 * jnp.cos(half)
    f = trial[6:7]
    return jnp.concatenate([v, r, trial[3:6], f, f * trial[7:8], f * trial[8:9]], axis=0)


def rows_of(x):
    n = x.shape[1] // 128
    return x.reshape(x.shape[0], n, 128).transpose(1, 0, 2).reshape(n * x.shape[0], 128)


def on_device(cameras, increment, points, gradient, inverse, cj, pj, observed, tb, tp, oc, op, accept):
    trial = cameras + increment
    inc_tab = lax.all_gather(increment, PTS_CAM, axis=0, tiled=True)
    cam_tab = lax.all_gather(camera_rows(trial), PTS_CAM, axis=0, tiled=True)
    oc2 = oc.reshape(-1, 128)
    op2 = op.reshape(-1, 128)
    reduced = reduce_points(inc_tab, cj, pj, oc2, op2, tb, tp, points.shape[1])
    reduced = lax.psum(reduced, CAM)
    d = gradient - reduced
    step = jnp.stack([inverse[3*i]*d[0] + inverse[3*i+1]*d[1] + inverse[3*i+2]*d[2] for i in range(3)])
    new = points + step
    pts_tab = rows_of(jnp.concatenate([new, jnp.zeros_like(new[0:1])], axis=0))
    res, cost = project_points(cam_tab, pts_tab, oc2, op2, rows_of(observed), tb, tp)
    n = observed.shape[1]
    residual = res.reshape(n // 128, 2, 128).transpose(1, 0, 2).reshape(2, n)
    total = lax.psum(jnp.sum(cost), PTS_CAM)
    flag = jnp.remainder(accept, 2).astype(F32)
    return (residual, total / (2.0 * n * lax.axis_size(PTS_CAM)), points + flag * step, cameras + flag * increment)


def solution(mesh):
    split = Mesh(mesh.devices.reshape(4, 4, 2, mesh.shape["cam"]), PTS_CAM)
    in_specs = (P(None, PTS_CAM), P(None, PTS_CAM), P(None, PTS), P(None, PTS), P(None, PTS),
                P(None, PTS_CAM), P(None, PTS_CAM), P(None, PTS_CAM),
                P(PTS_CAM), P(PTS_CAM), P(PTS_CAM), P(PTS_CAM), P())
    out_specs = (P(None, PTS_CAM), P(), P(None, PTS), P(None, PTS_CAM))
    return jax.shard_map(on_device, mesh=split, in_specs=in_specs, out_specs=out_specs, check_vma=False)
```

```python
import functools, math
import jax, jax.numpy as jnp
from jax import lax
from jax.experimental import pallas as pl
from jax.experimental.pallas import tpu as pltpu
from jax.sharding import Mesh
from jax.sharding import PartitionSpec as P

CB=128; PB=256; TILE=256
F32=jnp.float32
GROUP=1024
TPG=GROUP//TILE

def lane_gather(table, index):
    return lax.gather(table, index[..., None],
        lax.GatherDimensionNumbers(offset_dims=(), collapsed_slice_dims=(1,), start_index_map=(1,),
            operand_batching_dims=(0,), start_indices_batching_dims=(0,)),
        slice_sizes=(1,1), mode=lax.GatherScatterMode.PROMISE_IN_BOUNDS)

def tile_rows(rows, row_id):
    a,b,c,d = rows
    return jnp.where(row_id<4, jnp.where(row_id<2,a,b), jnp.where(row_id<6,c,d))

def spread(ref, first):
    return ref[pl.ds(first, 8, stride=0), :]

PH=8; PL=32
UN=8

def reduce_body(chunk, blocks_n, tb, tp, word, inc_ref, cj_ref, pj_ref, oc_ref, op_ref, cam_ref, own_ref, out_ref, kept_ref, acc, jscr, pscr, wscr):
    step = pl.program_id(0)
    groups = chunk//GROUP
    row_id = lax.broadcasted_iota(jnp.int32,(8,128),0)
    @pl.when(step==0)
    def _():
        def zero(i,_):
            acc[pl.ds(pl.multiple_of(i*(PH*8),PH*8),PH*8),:] = jnp.zeros((PH*8,PL),F32)
            return 0
        lax.fori_loop(0, blocks_n, zero, 0, unroll=8)
        wscr[...] = jnp.zeros_like(wscr)
        kept_ref[...] = cam_ref[...] + (word[0] & 1).astype(F32)*own_ref[...]
    def couple(g, slot):
        base = step*(chunk//TILE) + g*TPG
        cams = [tb[base+i]*9 for i in range(TPG)]
        cam = oc_ref[pl.ds(pl.multiple_of(g*8,8),8),:]
        for j in range(8):
            at = pl.ds(pl.multiple_of(g*GROUP+j*128,128),128)
            jscr[slot, j*24:j*24+18,:] = cj_ref[:,at].astype(F32)
            pscr[slot, j*8:j*8+6,:] = pj_ref[:,at].astype(F32)
        first=second=None
        for m in range(9):
            t = tile_rows([spread(inc_ref, c+m) for c in cams], row_id)
            v = lane_gather(t, cam)
            a = jscr[slot, pl.ds(m,8,stride=24),:]*v
            b = jscr[slot, pl.ds(9+m,8,stride=24),:]*v
            first = a if first is None else first+a
            second = b if second is None else second+b
        for n in range(3):
            v = pscr[slot, pl.ds(n,8,stride=8),:]*first + pscr[slot, pl.ds(3+n,8,stride=8),:]*second
            hi = v.astype(jnp.bfloat16).astype(F32)
            wscr[slot, pl.ds(n,8,stride=8),:] = hi
            wscr[slot, pl.ds(3+n,8,stride=8),:] = v-hi
    def scatter(g, slot):
        base = step*(chunk//TILE) + g*TPG
        for t in range(TPG):
            lhs=[]; rhs=[]
            for h in range(2):
                s=2*t+h
                w = wscr[slot, s*8:s*8+8,:]
                ids = op_ref[pl.ds(g*8+s,8,stride=0),:]
                hi = lax.shift_right_logical(ids,PL.bit_length()-1)
                lo = ids & (PL-1)
                lhs.append(jnp.concatenate([jnp.where(hi==k,w,0.0) for k in range(PH)],axis=0).astype(jnp.bfloat16))
                rhs.append(jnp.concatenate([jnp.where(lo-8*k==row_id,1.0,0.0) for k in range(PL//8)],axis=0).astype(jnp.bfloat16))
            L=jnp.concatenate(lhs,axis=1); R=jnp.concatenate(rhs,axis=1)
            r = lax.dot_general(L,R,(((1,),(1,)),((),())),preferred_element_type=F32)
            at = pl.ds(pl.multiple_of(tp[base+t]*(PH*8),PH*8),PH*8)
            acc[at,:] += r
    def body(i,_):
        for u in range(UN): couple(i*UN+u, u)
        for u in range(UN): scatter(i*UN+u, u)
        return 0
    lax.fori_loop(0, groups//UN, body, 0)
    @pl.when(step==pl.num_programs(0)-1)
    def _():
        def flush(i,_):
            for h in range(2):
                n = 128//PL
                x = jnp.concatenate([acc[pl.ds(pl.multiple_of(i*(PH*8)+(h*n+k)*8,8),8),:] for k in range(n)],axis=1)
                s = x[0:3,:]+x[3:6,:]
                for n in range(3):
                    out_ref[n, pl.ds(2*i+h,1),:] = s[n:n+1,:]
            return 0
        lax.fori_loop(0, blocks_n, flush, 0, unroll=8)

def reduce_points(inc, cj, pj, oc, op, tb, tp, word, cameras, increment, npts, chunk=32768):
    n=cj.shape[1]
    blocks_n=npts//PB
    return pl.pallas_call(
        functools.partial(reduce_body, chunk, blocks_n),
        out_shape=(jax.ShapeDtypeStruct((3,npts//128,128),F32), jax.ShapeDtypeStruct((9,128),F32)),
        grid_spec=pltpu.PrefetchScalarGridSpec(
            num_scalar_prefetch=3, grid=(n//chunk,),
            in_specs=[
                pl.BlockSpec(inc.shape, lambda i,*_:(0,0)),
                pl.BlockSpec((18,chunk), lambda i,*_:(0,i)),
                pl.BlockSpec((6,chunk), lambda i,*_:(0,i)),
                pl.BlockSpec((chunk//128,128), lambda i,*_:(i,0)),
                pl.BlockSpec((chunk//128,128), lambda i,*_:(i,0)),
                pl.BlockSpec((9,128), lambda i,*_:(0,0)),
                pl.BlockSpec((9,128), lambda i,*_:(0,0)),
            ],
            out_specs=(pl.BlockSpec((3,npts//128,128), lambda i,*_:(0,0,0)), pl.BlockSpec((9,128), lambda i,*_:(0,0))),
            scratch_shapes=[pltpu.VMEM((blocks_n*PH*8,PL),F32), pltpu.VMEM((UN,192,128),F32), pltpu.VMEM((UN,64,128),F32), pltpu.VMEM((UN,64,128),F32)],
        ),
        compiler_params=pltpu.CompilerParams(dimension_semantics=("arbitrary",), vmem_limit_bytes=60*1024*1024),
        name="reduce_points",
    )(tb,tp,word,inc,cj,pj,oc,op,cameras,increment)

CT=10
def project_body(chunk, tb, tp, cam_ref, pts_ref, oc_ref, op_ref, ob_ref, res_ref, cost_ref):
    step=pl.program_id(0)
    groups=chunk//GROUP
    row_id=lax.broadcasted_iota(jnp.int32,(8,128),0)
    @pl.when(step==0)
    def _():
        cost_ref[...]=jnp.zeros_like(cost_ref)
    def one(g):
        base=step*(chunk//TILE)+g*TPG
        cams=[tb[base+i]*CT for i in range(TPG)]
        pts=[tp[base+i]*2 for i in range(TPG)]
        at8=pl.ds(pl.multiple_of(g*8,8),8)
        cam=oc_ref[at8,:]; pid=op_ref[at8,:]
        half=pts_ref.shape[0]//3
        upper=pid>=128; plow=pid&127
        def look(r): return lane_gather(tile_rows([spread(cam_ref,c+r) for c in cams],row_id),cam)
        def lookp(r):
            a=lane_gather(tile_rows([spread(pts_ref,p+r*half) for p in pts],row_id),plow)
            b=lane_gather(tile_rows([spread(pts_ref,p+r*half+1) for p in pts],row_id),plow)
            return jnp.where(upper,b,a)
        x,y,z=lookp(0),lookp(1),lookp(2)
        vx,vy,vz,r,t0,t1,t2,f0,f1,f2=[look(i) for i in range(CT)]
        ax=vy*z-vz*y; ay=vz*x-vx*z; az=vx*y-vy*x
        px=x+r*ax+(vy*az-vz*ay)+t0
        py=y+r*ay+(vz*ax-vx*az)+t1
        pz=z+r*az+(vx*ay-vy*ax)+t2
        inv=1.0/jnp.maximum(-pz,1.0)
        u=px*inv; v=py*inv
        q=u*u+v*v
        fac=f0+q*(f1+q*f2)
        o0=pl.ds(g*16,8,stride=2); o1=pl.ds(g*16+1,8,stride=2)
        ru=fac*u-ob_ref[o0,:]; rv=fac*v-ob_ref[o1,:]
        res_ref[o0,:]=ru; res_ref[o1,:]=rv
        return ru*ru+rv*rv
    def body(i,c):
        for u in range(8): c=c+one(i*8+u)
        return c
    cost_ref[...]+=lax.fori_loop(0,groups//8,body,jnp.zeros((8,128),F32))

def project_points(cam, pts, oc, op, ob, tb, tp, chunk=32768):
    n=oc.shape[0]*128
    return pl.pallas_call(
        functools.partial(project_body, chunk),
        out_shape=(jax.ShapeDtypeStruct((n//64,128),F32), jax.ShapeDtypeStruct((8,128),F32)),
        grid_spec=pltpu.PrefetchScalarGridSpec(
            num_scalar_prefetch=2, grid=(n//chunk,),
            in_specs=[
                pl.BlockSpec(cam.shape, lambda i,*_:(0,0)),
                pl.BlockSpec(pts.shape, lambda i,*_:(0,0)),
                pl.BlockSpec((chunk//128,128), lambda i,*_:(i,0)),
                pl.BlockSpec((chunk//128,128), lambda i,*_:(i,0)),
                pl.BlockSpec((chunk//64,128), lambda i,*_:(i,0)),
            ],
            out_specs=(pl.BlockSpec((chunk//64,128), lambda i,*_:(i,0)), pl.BlockSpec((8,128), lambda i,*_:(0,0))),
        ),
        compiler_params=pltpu.CompilerParams(dimension_semantics=("arbitrary",), vmem_limit_bytes=60*1024*1024),
        name="project_points",
    )(tb,tp,cam,pts,oc,op,ob)


MESH = pl.DeviceIdType.MESH
X, Y, CORE, CAM = "pts_0", "pts_1", "pts_2", "cam"
PTS = (X, Y, CORE)
PTS_CAM = PTS + (CAM,)


def peer(axis, hop):
    n = lax.axis_size(axis)
    return {axis: lax.rem(lax.axis_index(axis) + hop, n)}


def greet(peers):
    barrier = pltpu.get_barrier_semaphore()
    for p in peers:
        pl.semaphore_signal(barrier, inc=1, device_id=p, device_id_type=MESH)
    pl.semaphore_wait(barrier, len(peers))


def hops(axis):
    return range(1, lax.axis_size(axis))


def send(src, dst, send_sem, recv_sem, to):
    copy = pltpu.make_async_remote_copy(src, dst, send_sem, recv_sem, device_id=to, device_id_type=MESH)
    copy.start()
    return copy


def gather_body(local_ref, out_ref, local_sem, send_sem, recv_sem):
    at = {a: lax.axis_index(a) for a in (X, Y, CORE, CAM)}

    def part(k, whole):
        i = [slice(None) if a in whole else at[a] for a in (X, Y, CORE, CAM)]
        return out_ref.at[(*i, pl.ds(3 * k, 3))]

    own = out_ref.at[at[X], at[Y], at[CORE], at[CAM]]
    mine = pltpu.make_async_copy(local_ref, own, local_sem)
    mine.start()
    greet([peer(a, h) for a in (CAM, Y, X, CORE) for h in hops(a)])
    mine.wait()
    order = ((CAM, Y, X), (Y, X, CAM), (X, CAM, Y))
    slot = 0
    for stage in range(3):
        copies = []
        for h in hops(CAM):
            for k in range(3):
                axis, done = order[k][stage], order[k][:stage]
                copies.append(send(part(k, done), part(k, done), send_sem.at[slot], recv_sem.at[slot], peer(axis, h)))
                slot += 1
        for cp in copies:
            cp.wait()
    half = out_ref.at[:, :, at[CORE]]
    send(half, half, send_sem.at[slot], recv_sem.at[slot], peer(CORE, 1)).wait()


def gather_rows(local):
    rows = local.shape[0]
    nx, ny, nc, nz = [lax.axis_size(a) for a in (X, Y, CORE, CAM)]
    out = pl.pallas_call(
        gather_body,
        out_shape=jax.ShapeDtypeStruct((nx, ny, nc, nz, rows, 1, 128), F32),
        in_specs=[pl.BlockSpec(memory_space=pltpu.VMEM)],
        out_specs=pl.BlockSpec(memory_space=pltpu.VMEM),
        scratch_shapes=[pltpu.SemaphoreType.DMA, pltpu.SemaphoreType.DMA((28,)), pltpu.SemaphoreType.DMA((28,))],
        compiler_params=pltpu.CompilerParams(collective_id=0, has_side_effects=True),
        name="gather_rows",
    )(local.reshape(rows, 1, 128))
    return out.reshape(nx * ny * nc * nz * rows, 128)


def cost_peers():
    near = [{**peer(Y, i), **peer(CAM, j)} for i in range(4) for j in range(4) if i or j]
    far = [{**peer(X, i), **peer(CORE, j)} for i in range(4) for j in range(2) if i or j]
    return near, far


def cost_body(scale, part_ref, out_ref, buf, send_sem, recv_sem):
    x, y, c, z = [lax.axis_index(a) for a in (X, Y, CORE, CAM)]
    peers = cost_peers()
    greet(peers[0] + peers[1])
    value = part_ref[...]
    slot = 0
    for stage, (me, count) in enumerate(((y * 4 + z, 16), (x * 2 + c, 8))):
        buf[stage, pl.ds(pl.multiple_of(me * 8, 8), 8), :] = value
        own = buf.at[stage, pl.ds(pl.multiple_of(me * 8, 8), 8)]
        copies = []
        for p in peers[stage]:
            copies.append(send(own, own, send_sem.at[slot], recv_sem.at[slot], p))
            slot += 1
        for cp in copies:
            cp.wait()
        value = buf[stage, 0:8, :]
        for k in range(1, count):
            value = value + buf[stage, k * 8:k * 8 + 8, :]
    out_ref[...] = jnp.sum(value, axis=(0, 1), keepdims=True) * scale


def total_cost(part, scale):
    out = pl.pallas_call(
        functools.partial(cost_body, scale),
        out_shape=jax.ShapeDtypeStruct((1, 1), F32),
        in_specs=[pl.BlockSpec(memory_space=pltpu.VMEM)],
        out_specs=pl.BlockSpec(memory_space=pltpu.VMEM),
        scratch_shapes=[pltpu.VMEM((2, 128, 128), F32), pltpu.SemaphoreType.DMA((22,)), pltpu.SemaphoreType.DMA((22,))],
        compiler_params=pltpu.CompilerParams(collective_id=1, has_side_effects=True),
        name="total_cost",
    )(part)
    return out.reshape(())


RT2 = math.sqrt(2.0)


def camera_rows(trial):
    w = [trial[i:i + 1] for i in range(3)]
    half = 0.5 * jnp.sqrt(w[0] * w[0] + w[1] * w[1] + w[2] * w[2])
    zero = half == 0.0
    ratio = (0.5 * RT2) * jnp.where(zero, 1.0, jnp.sin(half) / jnp.where(zero, 1.0, half))
    f = trial[6:7]
    return [ratio * a for a in w] + [RT2 * jnp.cos(half), trial[3:4], trial[4:5], trial[5:6], f, f * trial[7:8], f * trial[8:9]]


def solve_body(red_ref, cam_ref, inc_ref, pts_hbm, grad_hbm, inv_hbm, new_ref, tab_ref, pts, grad, inv, pscr, gscr, iscr,
               far, near, total, local_sem, send_sem, recv_sem):
    cx, cy, cc = [lax.axis_index(a) for a in (X, Y, CORE)]
    z = lax.axis_index(CAM)
    n = lax.axis_size(CAM)
    rows = red_ref.shape[1] // n
    half = rows // 2
    lanes = pl.ds(pl.multiple_of(z * (rows * 128), 128), rows * 128)
    loads = [pltpu.make_async_copy(src.at[:, lanes], dst, local_sem.at[i])
             for i, (src, dst) in enumerate(((pts_hbm, pts), (grad_hbm, grad), (inv_hbm, inv)))]
    for cp in loads:
        cp.start()
    right, left = peer(CAM, 1), peer(CAM, n - 1)
    for i, row in enumerate(camera_rows(cam_ref[...] + inc_ref[...])):
        tab_ref[cx, cy, cc, z, i] = row
    greet([peer(a, h) for a in (CAM, Y, X, CORE) for h in hops(a)])

    def spread_table(axis, part, slot):
        return [send(part, part, send_sem.at[slot + h - 1], recv_sem.at[slot + h - 1], peer(axis, h)) for h in hops(axis)]

    table = spread_table(CAM, tab_ref.at[cx, cy, cc, z], 10)

    def at(k):
        return lax.rem(z + k, n) * rows

    a = send(red_ref.at[:, pl.ds(at(2), half)], far.at[0], send_sem.at[0], recv_sem.at[0], right)
    b = send(red_ref.at[:, pl.ds(at(2) + half, half)], far.at[1], send_sem.at[1], recv_sem.at[1], left)
    c = send(red_ref.at[:, pl.ds(at(1) + half, half)], near.at[0, :, pl.ds(half, half)], send_sem.at[2], recv_sem.at[2], right)
    d = send(red_ref.at[:, pl.ds(at(n - 1), half)], near.at[1, :, pl.ds(0, half)], send_sem.at[3], recv_sem.at[3], left)
    a.wait_recv()
    total[0] = red_ref[:, pl.ds(at(1), half), :] + far[0]
    e = send(total.at[0], near.at[0, :, pl.ds(0, half)], send_sem.at[4], recv_sem.at[4], right)
    b.wait_recv()
    total[1] = red_ref[:, pl.ds(at(n - 1) + half, half), :] + far[1]
    f = send(total.at[1], near.at[1, :, pl.ds(half, half)], send_sem.at[5], recv_sem.at[5], left)
    for cp in table:
        cp.wait()
    table = spread_table(Y, tab_ref.at[cx, cy, cc], 13)
    for cp in loads:
        cp.wait()
    c.wait_recv()
    d.wait_recv()
    e.wait_recv()
    f.wait_recv()

    def group(g, _):
        r8 = pl.ds(pl.multiple_of(g * 8, 8), 8)
        for j in range(8):
            l = pl.ds(pl.multiple_of(g * 1024 + j * 128, 128), 128)
            pscr[pl.ds(j * 8, 3), :] = pts[:, l]
            gscr[pl.ds(j * 8, 3), :] = grad[:, l]
            iscr[pl.ds(j * 16, 9), :] = inv[:, l]
        own = pl.ds(pl.multiple_of(z * rows + g * 8, 8), 8)
        res = [gscr[pl.ds(k, 8, stride=8), :]
               - (red_ref[k, own, :] + near[0, k, r8, :] + near[1, k, r8, :]) for k in range(3)]
        for i in range(3):
            step = (iscr[pl.ds(3 * i, 8, stride=16), :] * res[0] + iscr[pl.ds(3 * i + 1, 8, stride=16), :] * res[1]
                    + iscr[pl.ds(3 * i + 2, 8, stride=16), :] * res[2])
            new_ref[i, own, :] = pscr[pl.ds(i, 8, stride=8), :] + step
        return 0

    lax.fori_loop(0, rows // 8, group, 0)
    for cp in (a, b, c, d, e, f):
        cp.wait_send()
    for cp in table:
        cp.wait()
    table = spread_table(X, tab_ref.at[cx, :, cc], 16)
    own = new_ref.at[:, pl.ds(z * rows, rows)]
    g = send(own, own, send_sem.at[6], recv_sem.at[6], right)
    h = send(own, own, send_sem.at[7], recv_sem.at[7], left)
    g.wait_recv()
    first = new_ref.at[:, pl.ds(at(n - 1), half)]
    k = send(first, first, send_sem.at[8], recv_sem.at[8], right)
    h.wait_recv()
    second = new_ref.at[:, pl.ds(at(1) + half, half)]
    m = send(second, second, send_sem.at[9], recv_sem.at[9], left)
    for cp in table:
        cp.wait()
    table = spread_table(CORE, tab_ref.at[:, :, cc], 19)
    k.wait_recv()
    m.wait_recv()
    for cp in (g, h, k, m):
        cp.wait_send()
    for cp in table:
        cp.wait()


def solve_points(reduced, cameras, increment, points, gradient, inverse):
    rows = reduced.shape[1] // 4
    nx, ny, nc, nz = [lax.axis_size(a) for a in (X, Y, CORE, CAM)]
    hbm = pl.BlockSpec(memory_space=pl.ANY)
    vmem = pl.BlockSpec(memory_space=pltpu.VMEM)
    new, table = pl.pallas_call(
        solve_body,
        out_shape=(jax.ShapeDtypeStruct(reduced.shape, F32), jax.ShapeDtypeStruct((nx, ny, nc, nz, CT, 1, 128), F32)),
        in_specs=[vmem, vmem, vmem, hbm, hbm, hbm],
        out_specs=(vmem, vmem),
        scratch_shapes=[
            pltpu.VMEM((3, rows * 128), F32), pltpu.VMEM((3, rows * 128), F32), pltpu.VMEM((9, rows * 128), F32),
            pltpu.VMEM((64, 128), F32), pltpu.VMEM((64, 128), F32), pltpu.VMEM((128, 128), F32),
            pltpu.VMEM((2, 3, rows // 2, 128), F32), pltpu.VMEM((2, 3, rows, 128), F32),
            pltpu.VMEM((2, 3, rows // 2, 128), F32),
            pltpu.SemaphoreType.DMA((3,)), pltpu.SemaphoreType.DMA((20,)), pltpu.SemaphoreType.DMA((20,)),
        ],
        compiler_params=pltpu.CompilerParams(collective_id=2, has_side_effects=True, vmem_limit_bytes=60 * 1024 * 1024),
        name="solve_points",
    )(reduced, cameras, increment, points, gradient, inverse)
    return new, table.reshape(nx * ny * nc * nz * CT, 128)


def rows_of(x):
    n = x.shape[1] // 128
    return x.reshape(x.shape[0], n, 128).transpose(1, 0, 2).reshape(n * x.shape[0], 128)


def on_device(cameras, increment, points, gradient, inverse, cj, pj, observed, tb, tp, oc, op, accept):
    oc2 = oc.reshape(-1, 128)
    op2 = op.reshape(-1, 128)
    reduced, kept = reduce_points(gather_rows(increment), cj, pj, oc2, op2, tb, tp, accept.reshape(1), cameras, increment, points.shape[1])
    new, table = solve_points(reduced, cameras, increment, points, gradient, inverse)
    res, cost = project_points(table, new.reshape(-1, 128), oc2, op2, rows_of(observed), tb, tp)
    n = observed.shape[1]
    residual = res.reshape(n // 128, 2, 128).transpose(1, 0, 2).reshape(2, n)
    total = total_cost(cost, 1.0 / (2.0 * n * lax.axis_size(PTS_CAM)))
    accepted = jnp.where((accept & 1) == 1, new.reshape(3, -1), points)
    return residual, total, accepted, kept


def solution(mesh):
    split = Mesh(mesh.devices.reshape(4, 4, 2, mesh.shape["cam"]), PTS_CAM)
    in_specs = (P(None, PTS_CAM), P(None, PTS_CAM), P(None, PTS), P(None, PTS), P(None, PTS),
                P(None, PTS_CAM), P(None, PTS_CAM), P(None, PTS_CAM),
                P(PTS_CAM), P(PTS_CAM), P(PTS_CAM), P(PTS_CAM), P())
    out_specs = (P(None, PTS_CAM), P(), P(None, PTS), P(None, PTS_CAM))
    return jax.shard_map(on_device, mesh=split, in_specs=in_specs, out_specs=out_specs, check_vma=False)
```

```python
import functools, math
import jax, jax.numpy as jnp
from jax import lax
from jax.experimental import pallas as pl
from jax.experimental.pallas import tpu as pltpu
from jax.sharding import Mesh
from jax.sharding import PartitionSpec as P

CB=128; PB=256; TILE=256
F32=jnp.float32
GROUP=1024
TPG=GROUP//TILE

def lane_gather(table, index):
    return lax.gather(table, index[..., None],
        lax.GatherDimensionNumbers(offset_dims=(), collapsed_slice_dims=(1,), start_index_map=(1,),
            operand_batching_dims=(0,), start_indices_batching_dims=(0,)),
        slice_sizes=(1,1), mode=lax.GatherScatterMode.PROMISE_IN_BOUNDS)

def tile_rows(rows, row_id):
    a,b,c,d = rows
    return jnp.where(row_id<4, jnp.where(row_id<2,a,b), jnp.where(row_id<6,c,d))

def spread(ref, first):
    return ref[pl.ds(first, 8, stride=0), :]

PH=8; PL=32
UN=8

def reduce_body(chunk, blocks_n, tb, tp, word, inc_ref, cj_ref, pj_ref, oc_ref, op_ref, cam_ref, own_ref, out_ref, kept_ref, acc, jscr, pscr, wscr):
    step = pl.program_id(0)
    groups = chunk//GROUP
    row_id = lax.broadcasted_iota(jnp.int32,(8,128),0)
    @pl.when(step==0)
    def _():
        def zero(i,_):
            acc[pl.ds(pl.multiple_of(i*(PH*8),PH*8),PH*8),:] = jnp.zeros((PH*8,PL),F32)
            return 0
        lax.fori_loop(0, blocks_n, zero, 0, unroll=8)
        wscr[...] = jnp.zeros_like(wscr)
        kept_ref[...] = cam_ref[...] + (word[0] & 1).astype(F32)*own_ref[...]
    def couple(g, slot):
        base = step*(chunk//TILE) + g*TPG
        cams = [tb[base+i]*9 for i in range(TPG)]
        cam = oc_ref[pl.ds(pl.multiple_of(g*8,8),8),:]
        for j in range(8):
            at = pl.ds(pl.multiple_of(g*GROUP+j*128,128),128)
            jscr[slot, j*24:j*24+18,:] = cj_ref[:,at].astype(F32)
            pscr[slot, j*8:j*8+6,:] = pj_ref[:,at].astype(F32)
        first=second=None
        for m in range(9):
            t = tile_rows([spread(inc_ref, c+m) for c in cams], row_id)
            v = lane_gather(t, cam)
            a = jscr[slot, pl.ds(m,8,stride=24),:]*v
            b = jscr[slot, pl.ds(9+m,8,stride=24),:]*v
            first = a if first is None else first+a
            second = b if second is None else second+b
        for n in range(3):
            v = pscr[slot, pl.ds(n,8,stride=8),:]*first + pscr[slot, pl.ds(3+n,8,stride=8),:]*second
            hi = v.astype(jnp.bfloat16).astype(F32)
            wscr[slot, pl.ds(n,8,stride=8),:] = hi
            wscr[slot, pl.ds(3+n,8,stride=8),:] = v-hi
    def scatter(g, slot):
        base = step*(chunk//TILE) + g*TPG
        for t in range(TPG):
            lhs=[]; rhs=[]
            for h in range(2):
                s=2*t+h
                w = wscr[slot, s*8:s*8+8,:]
                ids = op_ref[pl.ds(g*8+s,8,stride=0),:]
                hi = lax.shift_right_logical(ids,PL.bit_length()-1)
                lo = ids & (PL-1)
                lhs.append(jnp.concatenate([jnp.where(hi==k,w,0.0) for k in range(PH)],axis=0).astype(jnp.bfloat16))
                rhs.append(jnp.concatenate([jnp.where(lo-8*k==row_id,1.0,0.0) for k in range(PL//8)],axis=0).astype(jnp.bfloat16))
            L=jnp.concatenate(lhs,axis=1); R=jnp.concatenate(rhs,axis=1)
            r = lax.dot_general(L,R,(((1,),(1,)),((),())),preferred_element_type=F32)
            at = pl.ds(pl.multiple_of(tp[base+t]*(PH*8),PH*8),PH*8)
            acc[at,:] += r
    def body(i,_):
        for u in range(UN): couple(i*UN+u, u)
        for u in range(UN): scatter(i*UN+u, u)
        return 0
    lax.fori_loop(0, groups//UN, body, 0)
    @pl.when(step==pl.num_programs(0)-1)
    def _():
        def flush(i,_):
            for h in range(2):
                n = 128//PL
                x = jnp.concatenate([acc[pl.ds(pl.multiple_of(i*(PH*8)+(h*n+k)*8,8),8),:] for k in range(n)],axis=1)
                s = x[0:3,:]+x[3:6,:]
                for n in range(3):
                    out_ref[n, pl.ds(2*i+h,1),:] = s[n:n+1,:]
            return 0
        lax.fori_loop(0, blocks_n, flush, 0, unroll=8)

def reduce_points(inc, cj, pj, oc, op, tb, tp, word, cameras, increment, npts, chunk=16384):
    n=cj.shape[1]
    blocks_n=npts//PB
    return pl.pallas_call(
        functools.partial(reduce_body, chunk, blocks_n),
        out_shape=(jax.ShapeDtypeStruct((3,npts//128,128),F32), jax.ShapeDtypeStruct((9,128),F32)),
        grid_spec=pltpu.PrefetchScalarGridSpec(
            num_scalar_prefetch=3, grid=(n//chunk,),
            in_specs=[
                pl.BlockSpec(inc.shape, lambda i,*_:(0,0)),
                pl.BlockSpec((18,chunk), lambda i,*_:(0,i)),
                pl.BlockSpec((6,chunk), lambda i,*_:(0,i)),
                pl.BlockSpec((chunk//128,128), lambda i,*_:(i,0)),
                pl.BlockSpec((chunk//128,128), lambda i,*_:(i,0)),
                pl.BlockSpec((9,128), lambda i,*_:(0,0)),
                pl.BlockSpec((9,128), lambda i,*_:(0,0)),
            ],
            out_specs=(pl.BlockSpec((3,npts//128,128), lambda i,*_:(0,0,0)), pl.BlockSpec((9,128), lambda i,*_:(0,0))),
            scratch_shapes=[pltpu.VMEM((blocks_n*PH*8,PL),F32), pltpu.VMEM((UN,192,128),F32), pltpu.VMEM((UN,64,128),F32), pltpu.VMEM((UN,64,128),F32)],
        ),
        compiler_params=pltpu.CompilerParams(dimension_semantics=("arbitrary",), vmem_limit_bytes=60*1024*1024),
        name="reduce_points",
    )(tb,tp,word,inc,cj,pj,oc,op,cameras,increment)

CT=10
def project_body(chunk, tb, tp, cam_ref, pts_ref, oc_ref, op_ref, ob_ref, res_ref, cost_ref):
    step=pl.program_id(0)
    groups=chunk//GROUP
    row_id=lax.broadcasted_iota(jnp.int32,(8,128),0)
    @pl.when(step==0)
    def _():
        cost_ref[...]=jnp.zeros_like(cost_ref)
    def one(g):
        base=step*(chunk//TILE)+g*TPG
        cams=[tb[base+i]*CT for i in range(TPG)]
        pts=[tp[base+i]*2 for i in range(TPG)]
        at8=pl.ds(pl.multiple_of(g*8,8),8)
        cam=oc_ref[at8,:]; pid=op_ref[at8,:]
        half=pts_ref.shape[0]//3
        upper=pid>=128; plow=pid&127
        def look(r): return lane_gather(tile_rows([spread(cam_ref,c+r) for c in cams],row_id),cam)
        def lookp(r):
            a=lane_gather(tile_rows([spread(pts_ref,p+r*half) for p in pts],row_id),plow)
            b=lane_gather(tile_rows([spread(pts_ref,p+r*half+1) for p in pts],row_id),plow)
            return jnp.where(upper,b,a)
        x,y,z=lookp(0),lookp(1),lookp(2)
        vx,vy,vz,r,t0,t1,t2,f0,f1,f2=[look(i) for i in range(CT)]
        ax=vy*z-vz*y; ay=vz*x-vx*z; az=vx*y-vy*x
        px=x+r*ax+(vy*az-vz*ay)+t0
        py=y+r*ay+(vz*ax-vx*az)+t1
        pz=z+r*az+(vx*ay-vy*ax)+t2
        inv=1.0/jnp.maximum(-pz,1.0)
        u=px*inv; v=py*inv
        q=u*u+v*v
        fac=f0+q*(f1+q*f2)
        o0=pl.ds(g*16,8,stride=2); o1=pl.ds(g*16+1,8,stride=2)
        ru=fac*u-ob_ref[o0,:]; rv=fac*v-ob_ref[o1,:]
        res_ref[o0,:]=ru; res_ref[o1,:]=rv
        return ru*ru+rv*rv
    def body(i,c):
        for u in range(8): c=c+one(i*8+u)
        return c
    cost_ref[...]+=lax.fori_loop(0,groups//8,body,jnp.zeros((8,128),F32))

def project_points(cam, pts, oc, op, ob, tb, tp, chunk=32768):
    n=oc.shape[0]*128
    return pl.pallas_call(
        functools.partial(project_body, chunk),
        out_shape=(jax.ShapeDtypeStruct((n//64,128),F32), jax.ShapeDtypeStruct((8,128),F32)),
        grid_spec=pltpu.PrefetchScalarGridSpec(
            num_scalar_prefetch=2, grid=(n//chunk,),
            in_specs=[
                pl.BlockSpec(cam.shape, lambda i,*_:(0,0)),
                pl.BlockSpec(pts.shape, lambda i,*_:(0,0)),
                pl.BlockSpec((chunk//128,128), lambda i,*_:(i,0)),
                pl.BlockSpec((chunk//128,128), lambda i,*_:(i,0)),
                pl.BlockSpec((chunk//64,128), lambda i,*_:(i,0)),
            ],
            out_specs=(pl.BlockSpec((chunk//64,128), lambda i,*_:(i,0)), pl.BlockSpec((8,128), lambda i,*_:(0,0))),
        ),
        compiler_params=pltpu.CompilerParams(dimension_semantics=("arbitrary",), vmem_limit_bytes=60*1024*1024),
        name="project_points",
    )(tb,tp,cam,pts,oc,op,ob)


MESH = pl.DeviceIdType.MESH
X, Y, CORE, CAM = "pts_0", "pts_1", "pts_2", "cam"
PTS = (X, Y, CORE)
PTS_CAM = PTS + (CAM,)


def peer(axis, hop):
    n = lax.axis_size(axis)
    return {axis: lax.rem(lax.axis_index(axis) + hop, n)}


def greet(peers):
    barrier = pltpu.get_barrier_semaphore()
    for p in peers:
        pl.semaphore_signal(barrier, inc=1, device_id=p, device_id_type=MESH)
    pl.semaphore_wait(barrier, len(peers))


def hops(axis):
    return range(1, lax.axis_size(axis))


def send(src, dst, send_sem, recv_sem, to):
    copy = pltpu.make_async_remote_copy(src, dst, send_sem, recv_sem, device_id=to, device_id_type=MESH)
    copy.start()
    return copy


def gather_body(local_ref, out_ref, send_sem, recv_sem):
    at = {a: lax.axis_index(a) for a in (X, Y, CORE, CAM)}

    def part(k, whole):
        i = [slice(None) if a in whole else at[a] for a in (X, Y, CORE, CAM)]
        return out_ref.at[(*i, pl.ds(3 * k, 3))]

    for i in range(9):
        out_ref[at[X], at[Y], at[CORE], at[CAM], i] = local_ref[i:i + 1, :]
    greet([peer(a, h) for a in (CAM, Y, X, CORE) for h in hops(a)])
    order = ((CAM, Y, X), (Y, X, CAM), (X, CAM, Y))
    slot = 0
    for stage in range(3):
        copies = []
        for h in hops(CAM):
            for k in range(3):
                axis, done = order[k][stage], order[k][:stage]
                copies.append(send(part(k, done), part(k, done), send_sem.at[slot], recv_sem.at[slot], peer(axis, h)))
                slot += 1
        for cp in copies:
            cp.wait()
    half = out_ref.at[:, :, at[CORE]]
    send(half, half, send_sem.at[slot], recv_sem.at[slot], peer(CORE, 1)).wait()


def gather_rows(local):
    rows = local.shape[0]
    nx, ny, nc, nz = [lax.axis_size(a) for a in (X, Y, CORE, CAM)]
    out = pl.pallas_call(
        gather_body,
        out_shape=jax.ShapeDtypeStruct((nx, ny, nc, nz, rows, 1, 128), F32),
        in_specs=[pl.BlockSpec(memory_space=pltpu.VMEM)],
        out_specs=pl.BlockSpec(memory_space=pltpu.VMEM),
        scratch_shapes=[pltpu.SemaphoreType.DMA((28,)), pltpu.SemaphoreType.DMA((28,))],
        compiler_params=pltpu.CompilerParams(collective_id=0, has_side_effects=True),
        name="gather_rows",
    )(local)
    return out.reshape(nx * ny * nc * nz * rows, 128)


def cost_peers():
    near = [{**peer(Y, i), **peer(CAM, j)} for i in range(4) for j in range(4) if i or j]
    far = [{**peer(X, i), **peer(CORE, j)} for i in range(4) for j in range(2) if i or j]
    return near, far


def cost_body(scale, part_ref, out_ref, buf, send_sem, recv_sem):
    x, y, c, z = [lax.axis_index(a) for a in (X, Y, CORE, CAM)]
    peers = cost_peers()
    greet(peers[0] + peers[1])
    value = part_ref[...]
    slot = 0
    for stage, (me, count) in enumerate(((y * 4 + z, 16), (x * 2 + c, 8))):
        buf[stage, pl.ds(pl.multiple_of(me * 8, 8), 8), :] = value
        own = buf.at[stage, pl.ds(pl.multiple_of(me * 8, 8), 8)]
        copies = []
        for p in peers[stage]:
            copies.append(send(own, own, send_sem.at[slot], recv_sem.at[slot], p))
            slot += 1
        for cp in copies:
            cp.wait()
        value = buf[stage, 0:8, :]
        for k in range(1, count):
            value = value + buf[stage, k * 8:k * 8 + 8, :]
    out_ref[...] = jnp.sum(value, axis=(0, 1), keepdims=True) * scale


def total_cost(part, scale):
    out = pl.pallas_call(
        functools.partial(cost_body, scale),
        out_shape=jax.ShapeDtypeStruct((1, 1), F32),
        in_specs=[pl.BlockSpec(memory_space=pltpu.VMEM)],
        out_specs=pl.BlockSpec(memory_space=pltpu.VMEM),
        scratch_shapes=[pltpu.VMEM((2, 128, 128), F32), pltpu.SemaphoreType.DMA((22,)), pltpu.SemaphoreType.DMA((22,))],
        compiler_params=pltpu.CompilerParams(collective_id=1, has_side_effects=True),
        name="total_cost",
    )(part)
    return out.reshape(())


RT2 = math.sqrt(2.0)


def camera_rows(trial):
    w = [trial[i:i + 1] for i in range(3)]
    half = 0.5 * jnp.sqrt(w[0] * w[0] + w[1] * w[1] + w[2] * w[2])
    zero = half == 0.0
    ratio = (0.5 * RT2) * jnp.where(zero, 1.0, jnp.sin(half) / jnp.where(zero, 1.0, half))
    f = trial[6:7]
    return [ratio * a for a in w] + [RT2 * jnp.cos(half), trial[3:4], trial[4:5], trial[5:6], f, f * trial[7:8], f * trial[8:9]]


def solve_body(red_ref, cam_ref, inc_ref, pts_hbm, grad_hbm, inv_hbm, new_ref, tab_ref, pts, grad, inv, pscr, gscr, iscr,
               far, near, total, local_sem, send_sem, recv_sem):
    cx, cy, cc = [lax.axis_index(a) for a in (X, Y, CORE)]
    z = lax.axis_index(CAM)
    n = lax.axis_size(CAM)
    rows = red_ref.shape[1] // n
    half = rows // 2
    lanes = pl.ds(pl.multiple_of(z * (rows * 128), 128), rows * 128)
    loads = [pltpu.make_async_copy(src.at[:, lanes], dst, local_sem.at[i])
             for i, (src, dst) in enumerate(((pts_hbm, pts), (grad_hbm, grad), (inv_hbm, inv)))]
    for cp in loads:
        cp.start()
    right, left = peer(CAM, 1), peer(CAM, n - 1)
    for i, row in enumerate(camera_rows(cam_ref[...] + inc_ref[...])):
        tab_ref[cx, cy, cc, z, i] = row
    greet([peer(a, h) for a in (CAM, Y, X, CORE) for h in hops(a)])

    def spread_table(axis, part, slot):
        return [send(part, part, send_sem.at[slot + h - 1], recv_sem.at[slot + h - 1], peer(axis, h)) for h in hops(axis)]

    table = spread_table(CAM, tab_ref.at[cx, cy, cc, z], 10)

    def at(k):
        return lax.rem(z + k, n) * rows

    a = send(red_ref.at[:, pl.ds(at(2), half)], far.at[0], send_sem.at[0], recv_sem.at[0], right)
    b = send(red_ref.at[:, pl.ds(at(2) + half, half)], far.at[1], send_sem.at[1], recv_sem.at[1], left)
    c = send(red_ref.at[:, pl.ds(at(1) + half, half)], near.at[0, :, pl.ds(half, half)], send_sem.at[2], recv_sem.at[2], right)
    d = send(red_ref.at[:, pl.ds(at(n - 1), half)], near.at[1, :, pl.ds(0, half)], send_sem.at[3], recv_sem.at[3], left)
    a.wait_recv()
    total[0] = red_ref[:, pl.ds(at(1), half), :] + far[0]
    e = send(total.at[0], near.at[0, :, pl.ds(0, half)], send_sem.at[4], recv_sem.at[4], right)
    b.wait_recv()
    total[1] = red_ref[:, pl.ds(at(n - 1) + half, half), :] + far[1]
    f = send(total.at[1], near.at[1, :, pl.ds(half, half)], send_sem.at[5], recv_sem.at[5], left)
    for cp in table:
        cp.wait()
    table = spread_table(Y, tab_ref.at[cx, cy, cc], 13)
    for cp in loads:
        cp.wait()
    c.wait_recv()
    d.wait_recv()
    e.wait_recv()
    f.wait_recv()

    def group(g, _):
        r8 = pl.ds(pl.multiple_of(g * 8, 8), 8)
        for j in range(8):
            l = pl.ds(pl.multiple_of(g * 1024 + j * 128, 128), 128)
            pscr[pl.ds(j * 8, 3), :] = pts[:, l]
            gscr[pl.ds(j * 8, 3), :] = grad[:, l]
            iscr[pl.ds(j * 16, 9), :] = inv[:, l]
        own = pl.ds(pl.multiple_of(z * rows + g * 8, 8), 8)
        res = [gscr[pl.ds(k, 8, stride=8), :]
               - (red_ref[k, own, :] + near[0, k, r8, :] + near[1, k, r8, :]) for k in range(3)]
        for i in range(3):
            step = (iscr[pl.ds(3 * i, 8, stride=16), :] * res[0] + iscr[pl.ds(3 * i + 1, 8, stride=16), :] * res[1]
                    + iscr[pl.ds(3 * i + 2, 8, stride=16), :] * res[2])
            new_ref[i, own, :] = pscr[pl.ds(i, 8, stride=8), :] + step
        return 0

    def own(part):
        return new_ref.at[:, pl.ds(z * rows + part * half, half)]

    lax.fori_loop(0, half // 8, group, 0)
    g = send(own(0), own(0), send_sem.at[6], recv_sem.at[6], right)
    lax.fori_loop(half // 8, rows // 8, group, 0)
    h = send(own(1), own(1), send_sem.at[7], recv_sem.at[7], left)
    g2 = send(own(1), own(1), send_sem.at[8], recv_sem.at[8], right)
    h2 = send(own(0), own(0), send_sem.at[9], recv_sem.at[9], left)
    for cp in table:
        cp.wait()
    table = spread_table(X, tab_ref.at[cx, :, cc], 16)
    g.wait_recv()
    first = new_ref.at[:, pl.ds(at(n - 1), half)]
    k = send(first, first, send_sem.at[20], recv_sem.at[20], right)
    h.wait_recv()
    second = new_ref.at[:, pl.ds(at(1) + half, half)]
    m = send(second, second, send_sem.at[21], recv_sem.at[21], left)
    for cp in table:
        cp.wait()
    table = spread_table(CORE, tab_ref.at[:, :, cc], 19)
    for cp in (g2, h2, k, m):
        cp.wait_recv()
    for cp in (a, b, c, d, e, f, g, h, g2, h2, k, m):
        cp.wait_send()
    for cp in table:
        cp.wait()


def solve_points(reduced, cameras, increment, points, gradient, inverse):
    rows = reduced.shape[1] // 4
    nx, ny, nc, nz = [lax.axis_size(a) for a in (X, Y, CORE, CAM)]
    hbm = pl.BlockSpec(memory_space=pl.ANY)
    vmem = pl.BlockSpec(memory_space=pltpu.VMEM)
    new, table = pl.pallas_call(
        solve_body,
        out_shape=(jax.ShapeDtypeStruct(reduced.shape, F32), jax.ShapeDtypeStruct((nx, ny, nc, nz, CT, 1, 128), F32)),
        in_specs=[vmem, vmem, vmem, hbm, hbm, hbm],
        out_specs=(vmem, vmem),
        scratch_shapes=[
            pltpu.VMEM((3, rows * 128), F32), pltpu.VMEM((3, rows * 128), F32), pltpu.VMEM((9, rows * 128), F32),
            pltpu.VMEM((64, 128), F32), pltpu.VMEM((64, 128), F32), pltpu.VMEM((128, 128), F32),
            pltpu.VMEM((2, 3, rows // 2, 128), F32), pltpu.VMEM((2, 3, rows, 128), F32),
            pltpu.VMEM((2, 3, rows // 2, 128), F32),
            pltpu.SemaphoreType.DMA((3,)), pltpu.SemaphoreType.DMA((22,)), pltpu.SemaphoreType.DMA((22,)),
        ],
        compiler_params=pltpu.CompilerParams(collective_id=2, has_side_effects=True, vmem_limit_bytes=60 * 1024 * 1024),
        name="solve_points",
    )(reduced, cameras, increment, points, gradient, inverse)
    return new, table.reshape(nx * ny * nc * nz * CT, 128)


def rows_of(x):
    n = x.shape[1] // 128
    return x.reshape(x.shape[0], n, 128).transpose(1, 0, 2).reshape(n * x.shape[0], 128)


def on_device(cameras, increment, points, gradient, inverse, cj, pj, observed, tb, tp, oc, op, accept):
    oc2 = oc.reshape(-1, 128)
    op2 = op.reshape(-1, 128)
    reduced, kept = reduce_points(gather_rows(increment), cj, pj, oc2, op2, tb, tp, accept.reshape(1), cameras, increment, points.shape[1])
    new, table = solve_points(reduced, cameras, increment, points, gradient, inverse)
    res, cost = project_points(table, new.reshape(-1, 128), oc2, op2, rows_of(observed), tb, tp)
    n = observed.shape[1]
    residual = res.reshape(n // 128, 2, 128).transpose(1, 0, 2).reshape(2, n)
    total = total_cost(cost, 1.0 / (2.0 * n * lax.axis_size(PTS_CAM)))
    accepted = jnp.where((accept & 1) == 1, new.reshape(3, -1), points)
    return residual, total, accepted, kept


def solution(mesh):
    split = Mesh(mesh.devices.reshape(4, 4, 2, mesh.shape["cam"]), PTS_CAM)
    in_specs = (P(None, PTS_CAM), P(None, PTS_CAM), P(None, PTS), P(None, PTS), P(None, PTS),
                P(None, PTS_CAM), P(None, PTS_CAM), P(None, PTS_CAM),
                P(PTS_CAM), P(PTS_CAM), P(PTS_CAM), P(PTS_CAM), P())
    out_specs = (P(None, PTS_CAM), P(), P(None, PTS), P(None, PTS_CAM))
    return jax.shard_map(on_device, mesh=split, in_specs=in_specs, out_specs=out_specs, check_vma=False)
```

```python
import functools, math
import jax, jax.numpy as jnp
from jax import lax
from jax.experimental import pallas as pl
from jax.experimental.pallas import tpu as pltpu
from jax.sharding import Mesh
from jax.sharding import PartitionSpec as P

CB=128; PB=256; TILE=256
F32=jnp.float32
GROUP=1024
TPG=GROUP//TILE

def lane_gather(table, index):
    return lax.gather(table, index[..., None],
        lax.GatherDimensionNumbers(offset_dims=(), collapsed_slice_dims=(1,), start_index_map=(1,),
            operand_batching_dims=(0,), start_indices_batching_dims=(0,)),
        slice_sizes=(1,1), mode=lax.GatherScatterMode.PROMISE_IN_BOUNDS)

def tile_rows(rows, row_id):
    a,b,c,d = rows
    return jnp.where(row_id<4, jnp.where(row_id<2,a,b), jnp.where(row_id<6,c,d))

def spread(ref, first):
    return ref[pl.ds(first, 8, stride=0), :]

PH=8; PL=32
UN=16

def reduce_body(chunk, blocks_n, tb, tp, word, inc_ref, cj_ref, pj_ref, oc_ref, op_ref, cam_ref, own_ref, out_ref, kept_ref, acc, jscr, pscr, wscr):
    step = pl.program_id(0)
    groups = chunk//GROUP
    row_id = lax.broadcasted_iota(jnp.int32,(8,128),0)
    @pl.when(step==0)
    def _():
        def zero(i,_):
            acc[pl.ds(pl.multiple_of(i*(PH*8),PH*8),PH*8),:] = jnp.zeros((PH*8,PL),F32)
            return 0
        lax.fori_loop(0, blocks_n, zero, 0, unroll=8)
        wscr[...] = jnp.zeros_like(wscr)
        kept_ref[...] = cam_ref[...] + (word[0] & 1).astype(F32)*own_ref[...]
    def couple(g, slot):
        base = step*(chunk//TILE) + g*TPG
        cams = [tb[base+i]*9 for i in range(TPG)]
        cam = oc_ref[pl.ds(pl.multiple_of(g*8,8),8),:]
        for j in range(8):
            at = pl.ds(pl.multiple_of(g*GROUP+j*128,128),128)
            jscr[slot, j*24:j*24+18,:] = cj_ref[:,at].astype(F32)
            pscr[slot, j*8:j*8+6,:] = pj_ref[:,at].astype(F32)
        first=second=None
        for m in range(9):
            t = tile_rows([spread(inc_ref, c+m) for c in cams], row_id)
            v = lane_gather(t, cam)
            a = jscr[slot, pl.ds(m,8,stride=24),:]*v
            b = jscr[slot, pl.ds(9+m,8,stride=24),:]*v
            first = a if first is None else first+a
            second = b if second is None else second+b
        for n in range(3):
            v = pscr[slot, pl.ds(n,8,stride=8),:]*first + pscr[slot, pl.ds(3+n,8,stride=8),:]*second
            hi = v.astype(jnp.bfloat16).astype(F32)
            wscr[slot, pl.ds(n,8,stride=8),:] = hi
            wscr[slot, pl.ds(3+n,8,stride=8),:] = v-hi
    def scatter(g, slot):
        base = step*(chunk//TILE) + g*TPG
        for t in range(TPG):
            lhs=[]; rhs=[]
            for h in range(2):
                s=2*t+h
                w = wscr[slot, s*8:s*8+8,:]
                ids = op_ref[pl.ds(g*8+s,8,stride=0),:]
                hi = lax.shift_right_logical(ids,PL.bit_length()-1)
                lo = ids & (PL-1)
                lhs.append(jnp.concatenate([jnp.where(hi==k,w,0.0) for k in range(PH)],axis=0).astype(jnp.bfloat16))
                rhs.append(jnp.concatenate([jnp.where(lo-8*k==row_id,1.0,0.0) for k in range(PL//8)],axis=0).astype(jnp.bfloat16))
            L=jnp.concatenate(lhs,axis=1); R=jnp.concatenate(rhs,axis=1)
            r = lax.dot_general(L,R,(((1,),(1,)),((),())),preferred_element_type=F32)
            at = pl.ds(pl.multiple_of(tp[base+t]*(PH*8),PH*8),PH*8)
            acc[at,:] += r
    def body(i,_):
        for u in range(UN): couple(i*UN+u, u)
        for u in range(UN): scatter(i*UN+u, u)
        return 0
    lax.fori_loop(0, groups//UN, body, 0)
    @pl.when(step==pl.num_programs(0)-1)
    def _():
        def flush(i,_):
            for h in range(2):
                n = 128//PL
                x = jnp.concatenate([acc[pl.ds(pl.multiple_of(i*(PH*8)+(h*n+k)*8,8),8),:] for k in range(n)],axis=1)
                s = x[0:3,:]+x[3:6,:]
                for n in range(3):
                    out_ref[n, pl.ds(2*i+h,1),:] = s[n:n+1,:]
            return 0
        lax.fori_loop(0, blocks_n, flush, 0, unroll=32)

def reduce_points(inc, cj, pj, oc, op, tb, tp, word, cameras, increment, npts, chunk=16384):
    n=cj.shape[1]
    blocks_n=npts//PB
    return pl.pallas_call(
        functools.partial(reduce_body, chunk, blocks_n),
        out_shape=(jax.ShapeDtypeStruct((3,npts//128,128),F32), jax.ShapeDtypeStruct((9,128),F32)),
        grid_spec=pltpu.PrefetchScalarGridSpec(
            num_scalar_prefetch=3, grid=(n//chunk,),
            in_specs=[
                pl.BlockSpec(inc.shape, lambda i,*_:(0,0)),
                pl.BlockSpec((18,chunk), lambda i,*_:(0,i)),
                pl.BlockSpec((6,chunk), lambda i,*_:(0,i)),
                pl.BlockSpec((chunk//128,128), lambda i,*_:(i,0)),
                pl.BlockSpec((chunk//128,128), lambda i,*_:(i,0)),
                pl.BlockSpec((9,128), lambda i,*_:(0,0)),
                pl.BlockSpec((9,128), lambda i,*_:(0,0)),
            ],
            out_specs=(pl.BlockSpec((3,npts//128,128), lambda i,*_:(0,0,0)), pl.BlockSpec((9,128), lambda i,*_:(0,0))),
            scratch_shapes=[pltpu.VMEM((blocks_n*PH*8,PL),F32), pltpu.VMEM((UN,192,128),F32), pltpu.VMEM((UN,64,128),F32), pltpu.VMEM((UN,64,128),F32)],
        ),
        compiler_params=pltpu.CompilerParams(dimension_semantics=("arbitrary",), vmem_limit_bytes=60*1024*1024),
        name="reduce_points",
    )(tb,tp,word,inc,cj,pj,oc,op,cameras,increment)

CT=10
def project_body(chunk, tb, tp, cam_ref, pts_ref, oc_ref, op_ref, ob_ref, res_ref, cost_ref):
    step=pl.program_id(0)
    groups=chunk//GROUP
    row_id=lax.broadcasted_iota(jnp.int32,(8,128),0)
    @pl.when(step==0)
    def _():
        cost_ref[...]=jnp.zeros_like(cost_ref)
    def one(g):
        base=step*(chunk//TILE)+g*TPG
        cams=[tb[base+i]*CT for i in range(TPG)]
        pts=[tp[base+i]*2 for i in range(TPG)]
        at8=pl.ds(pl.multiple_of(g*8,8),8)
        cam=oc_ref[at8,:]; pid=op_ref[at8,:]
        half=pts_ref.shape[0]//3
        upper=pid>=128; plow=pid&127
        def look(r): return lane_gather(tile_rows([spread(cam_ref,c+r) for c in cams],row_id),cam)
        def lookp(r):
            a=lane_gather(tile_rows([spread(pts_ref,p+r*half) for p in pts],row_id),plow)
            b=lane_gather(tile_rows([spread(pts_ref,p+r*half+1) for p in pts],row_id),plow)
            return jnp.where(upper,b,a)
        x,y,z=lookp(0),lookp(1),lookp(2)
        vx,vy,vz,r,t0,t1,t2,f0,f1,f2=[look(i) for i in range(CT)]
        ax=vy*z-vz*y; ay=vz*x-vx*z; az=vx*y-vy*x
        px=x+r*ax+(vy*az-vz*ay)+t0
        py=y+r*ay+(vz*ax-vx*az)+t1
        pz=z+r*az+(vx*ay-vy*ax)+t2
        inv=1.0/jnp.maximum(-pz,1.0)
        u=px*inv; v=py*inv
        q=u*u+v*v
        fac=f0+q*(f1+q*f2)
        o0=pl.ds(g*16,8,stride=2); o1=pl.ds(g*16+1,8,stride=2)
        ru=fac*u-ob_ref[o0,:]; rv=fac*v-ob_ref[o1,:]
        res_ref[o0,:]=ru; res_ref[o1,:]=rv
        return ru*ru+rv*rv
    def body(i,c):
        for u in range(16): c=c+one(i*16+u)
        return c
    cost_ref[...]+=lax.fori_loop(0,groups//16,body,jnp.zeros((8,128),F32))

def project_points(cam, pts, oc, op, ob, tb, tp, chunk=65536):
    n=oc.shape[0]*128
    return pl.pallas_call(
        functools.partial(project_body, chunk),
        out_shape=(jax.ShapeDtypeStruct((n//64,128),F32), jax.ShapeDtypeStruct((8,128),F32)),
        grid_spec=pltpu.PrefetchScalarGridSpec(
            num_scalar_prefetch=2, grid=(n//chunk,),
            in_specs=[
                pl.BlockSpec(cam.shape, lambda i,*_:(0,0)),
                pl.BlockSpec(pts.shape, lambda i,*_:(0,0)),
                pl.BlockSpec((chunk//128,128), lambda i,*_:(i,0)),
                pl.BlockSpec((chunk//128,128), lambda i,*_:(i,0)),
                pl.BlockSpec((chunk//64,128), lambda i,*_:(i,0)),
            ],
            out_specs=(pl.BlockSpec((chunk//64,128), lambda i,*_:(i,0)), pl.BlockSpec((8,128), lambda i,*_:(0,0))),
        ),
        compiler_params=pltpu.CompilerParams(dimension_semantics=("arbitrary",), vmem_limit_bytes=60*1024*1024),
        name="project_points",
    )(tb,tp,cam,pts,oc,op,ob)


MESH = pl.DeviceIdType.MESH
X, Y, CORE, CAM = "pts_0", "pts_1", "pts_2", "cam"
PTS = (X, Y, CORE)
PTS_CAM = PTS + (CAM,)


def peer(axis, hop):
    n = lax.axis_size(axis)
    return {axis: lax.rem(lax.axis_index(axis) + hop, n)}


def greet(peers):
    barrier = pltpu.get_barrier_semaphore()
    for p in peers:
        pl.semaphore_signal(barrier, inc=1, device_id=p, device_id_type=MESH)
    pl.semaphore_wait(barrier, len(peers))


def hops(axis):
    return range(1, lax.axis_size(axis))


def send(src, dst, send_sem, recv_sem, to):
    copy = pltpu.make_async_remote_copy(src, dst, send_sem, recv_sem, device_id=to, device_id_type=MESH)
    copy.start()
    return copy


def gather_body(local_ref, out_ref, send_sem, recv_sem):
    at = {a: lax.axis_index(a) for a in (X, Y, CORE, CAM)}

    def part(k, whole):
        i = [slice(None) if a in whole else at[a] for a in (X, Y, CORE, CAM)]
        return out_ref.at[(*i, pl.ds(3 * k, 3))]

    for i in range(9):
        out_ref[at[X], at[Y], at[CORE], at[CAM], i] = local_ref[i:i + 1, :]
    greet([peer(a, h) for a in (CAM, Y, X, CORE) for h in hops(a)])
    order = ((CAM, Y, X), (Y, X, CAM), (X, CAM, Y))
    def start(k, stage):
        axis, done = order[k][stage], order[k][:stage]
        first = 9 * k + 3 * stage
        return [send(part(k, done), part(k, done), send_sem.at[first + h - 1], recv_sem.at[first + h - 1], peer(axis, h))
                for h in hops(axis)]

    sent = []
    flying = [start(k, 0) for k in range(3)]
    for stage in range(1, 4):
        for k in range(3):
            for cp in flying[k]:
                cp.wait_recv()
            sent += flying[k]
            if stage < 3:
                flying[k] = start(k, stage)
    half = out_ref.at[:, :, at[CORE]]
    last = send(half, half, send_sem.at[27], recv_sem.at[27], peer(CORE, 1))
    for cp in sent:
        cp.wait_send()
    last.wait()


def gather_rows(local):
    rows = local.shape[0]
    nx, ny, nc, nz = [lax.axis_size(a) for a in (X, Y, CORE, CAM)]
    out = pl.pallas_call(
        gather_body,
        out_shape=jax.ShapeDtypeStruct((nx, ny, nc, nz, rows, 1, 128), F32),
        in_specs=[pl.BlockSpec(memory_space=pltpu.VMEM)],
        out_specs=pl.BlockSpec(memory_space=pltpu.VMEM),
        scratch_shapes=[pltpu.SemaphoreType.DMA((28,)), pltpu.SemaphoreType.DMA((28,))],
        compiler_params=pltpu.CompilerParams(collective_id=0, has_side_effects=True),
        name="gather_rows",
    )(local)
    return out.reshape(nx * ny * nc * nz * rows, 128)


def cost_peers():
    near = [{**peer(Y, i), **peer(CAM, j)} for i in range(4) for j in range(4) if i or j]
    far = [{**peer(X, i), **peer(CORE, j)} for i in range(4) for j in range(2) if i or j]
    return near, far


def cost_body(scale, part_ref, out_ref, buf, send_sem, recv_sem):
    x, y, c, z = [lax.axis_index(a) for a in (X, Y, CORE, CAM)]
    peers = cost_peers()
    greet(peers[0] + peers[1])
    value = part_ref[...]
    slot = 0
    for stage, (me, count) in enumerate(((y * 4 + z, 16), (x * 2 + c, 8))):
        buf[stage, pl.ds(pl.multiple_of(me * 8, 8), 8), :] = value
        own = buf.at[stage, pl.ds(pl.multiple_of(me * 8, 8), 8)]
        copies = []
        for p in peers[stage]:
            copies.append(send(own, own, send_sem.at[slot], recv_sem.at[slot], p))
            slot += 1
        for cp in copies:
            cp.wait()
        value = buf[stage, 0:8, :]
        for k in range(1, count):
            value = value + buf[stage, k * 8:k * 8 + 8, :]
    out_ref[...] = jnp.sum(value, axis=(0, 1), keepdims=True) * scale


def total_cost(part, scale):
    out = pl.pallas_call(
        functools.partial(cost_body, scale),
        out_shape=jax.ShapeDtypeStruct((1, 1), F32),
        in_specs=[pl.BlockSpec(memory_space=pltpu.VMEM)],
        out_specs=pl.BlockSpec(memory_space=pltpu.VMEM),
        scratch_shapes=[pltpu.VMEM((2, 128, 128), F32), pltpu.SemaphoreType.DMA((22,)), pltpu.SemaphoreType.DMA((22,))],
        compiler_params=pltpu.CompilerParams(collective_id=1, has_side_effects=True),
        name="total_cost",
    )(part)
    return out.reshape(())


RT2 = math.sqrt(2.0)


def camera_rows(trial):
    w = [trial[i:i + 1] for i in range(3)]
    half = 0.5 * jnp.sqrt(w[0] * w[0] + w[1] * w[1] + w[2] * w[2])
    zero = half == 0.0
    ratio = (0.5 * RT2) * jnp.where(zero, 1.0, jnp.sin(half) / jnp.where(zero, 1.0, half))
    f = trial[6:7]
    return [ratio * a for a in w] + [RT2 * jnp.cos(half), trial[3:4], trial[4:5], trial[5:6], f, f * trial[7:8], f * trial[8:9]]


def solve_body(red_ref, cam_ref, inc_ref, pts_hbm, grad_hbm, inv_hbm, new_ref, tab_ref, pts, grad, inv, pscr, gscr, iscr,
               far, near, total, local_sem, send_sem, recv_sem):
    cx, cy, cc = [lax.axis_index(a) for a in (X, Y, CORE)]
    z = lax.axis_index(CAM)
    n = lax.axis_size(CAM)
    rows = red_ref.shape[1] // n
    half = rows // 2
    lanes = pl.ds(pl.multiple_of(z * (rows * 128), 128), rows * 128)
    loads = [pltpu.make_async_copy(src.at[:, lanes], dst, local_sem.at[i])
             for i, (src, dst) in enumerate(((pts_hbm, pts), (grad_hbm, grad), (inv_hbm, inv)))]
    for cp in loads:
        cp.start()
    right, left = peer(CAM, 1), peer(CAM, n - 1)
    for i, row in enumerate(camera_rows(cam_ref[...] + inc_ref[...])):
        tab_ref[cx, cy, cc, z, i] = row
    greet([peer(a, h) for a in (CAM, Y, X, CORE) for h in hops(a)])

    def spread_table(axis, part, slot):
        return [send(part, part, send_sem.at[slot + h - 1], recv_sem.at[slot + h - 1], peer(axis, h)) for h in hops(axis)]

    table = spread_table(CAM, tab_ref.at[cx, cy, cc, z], 10)

    def at(k):
        return lax.rem(z + k, n) * rows

    a = send(red_ref.at[:, pl.ds(at(2), half)], far.at[0], send_sem.at[0], recv_sem.at[0], right)
    b = send(red_ref.at[:, pl.ds(at(2) + half, half)], far.at[1], send_sem.at[1], recv_sem.at[1], left)
    c = send(red_ref.at[:, pl.ds(at(1) + half, half)], near.at[0, :, pl.ds(half, half)], send_sem.at[2], recv_sem.at[2], right)
    d = send(red_ref.at[:, pl.ds(at(n - 1), half)], near.at[1, :, pl.ds(0, half)], send_sem.at[3], recv_sem.at[3], left)
    a.wait_recv()
    total[0] = red_ref[:, pl.ds(at(1), half), :] + far[0]
    e = send(total.at[0], near.at[0, :, pl.ds(0, half)], send_sem.at[4], recv_sem.at[4], right)
    b.wait_recv()
    total[1] = red_ref[:, pl.ds(at(n - 1) + half, half), :] + far[1]
    f = send(total.at[1], near.at[1, :, pl.ds(half, half)], send_sem.at[5], recv_sem.at[5], left)
    for cp in table:
        cp.wait()
    table = spread_table(Y, tab_ref.at[cx, cy, cc], 13)
    for cp in loads:
        cp.wait()
    c.wait_recv()
    d.wait_recv()
    e.wait_recv()
    f.wait_recv()

    def group(g, _):
        r8 = pl.ds(pl.multiple_of(g * 8, 8), 8)
        for j in range(8):
            l = pl.ds(pl.multiple_of(g * 1024 + j * 128, 128), 128)
            pscr[pl.ds(j * 8, 3), :] = pts[:, l]
            gscr[pl.ds(j * 8, 3), :] = grad[:, l]
            iscr[pl.ds(j * 16, 9), :] = inv[:, l]
        own = pl.ds(pl.multiple_of(z * rows + g * 8, 8), 8)
        res = [gscr[pl.ds(k, 8, stride=8), :]
               - (red_ref[k, own, :] + near[0, k, r8, :] + near[1, k, r8, :]) for k in range(3)]
        for i in range(3):
            step = (iscr[pl.ds(3 * i, 8, stride=16), :] * res[0] + iscr[pl.ds(3 * i + 1, 8, stride=16), :] * res[1]
                    + iscr[pl.ds(3 * i + 2, 8, stride=16), :] * res[2])
            new_ref[i, own, :] = pscr[pl.ds(i, 8, stride=8), :] + step
        return 0

    def own(part):
        return new_ref.at[:, pl.ds(z * rows + part * half, half)]

    lax.fori_loop(0, half // 8, group, 0)
    g = send(own(0), own(0), send_sem.at[6], recv_sem.at[6], right)
    lax.fori_loop(half // 8, rows // 8, group, 0)
    h = send(own(1), own(1), send_sem.at[7], recv_sem.at[7], left)
    g2 = send(own(1), own(1), send_sem.at[8], recv_sem.at[8], right)
    h2 = send(own(0), own(0), send_sem.at[9], recv_sem.at[9], left)
    for cp in table:
        cp.wait()
    table = spread_table(X, tab_ref.at[cx, :, cc], 16)
    g.wait_recv()
    first = new_ref.at[:, pl.ds(at(n - 1), half)]
    k = send(first, first, send_sem.at[20], recv_sem.at[20], right)
    h.wait_recv()
    second = new_ref.at[:, pl.ds(at(1) + half, half)]
    m = send(second, second, send_sem.at[21], recv_sem.at[21], left)
    for cp in table:
        cp.wait()
    table = spread_table(CORE, tab_ref.at[:, :, cc], 19)
    for cp in (g2, h2, k, m):
        cp.wait_recv()
    for cp in (a, b, c, d, e, f, g, h, g2, h2, k, m):
        cp.wait_send()
    for cp in table:
        cp.wait()


def solve_points(reduced, cameras, increment, points, gradient, inverse):
    rows = reduced.shape[1] // 4
    nx, ny, nc, nz = [lax.axis_size(a) for a in (X, Y, CORE, CAM)]
    hbm = pl.BlockSpec(memory_space=pl.ANY)
    vmem = pl.BlockSpec(memory_space=pltpu.VMEM)
    new, table = pl.pallas_call(
        solve_body,
        out_shape=(jax.ShapeDtypeStruct(reduced.shape, F32), jax.ShapeDtypeStruct((nx, ny, nc, nz, CT, 1, 128), F32)),
        in_specs=[vmem, vmem, vmem, hbm, hbm, hbm],
        out_specs=(vmem, vmem),
        scratch_shapes=[
            pltpu.VMEM((3, rows * 128), F32), pltpu.VMEM((3, rows * 128), F32), pltpu.VMEM((9, rows * 128), F32),
            pltpu.VMEM((64, 128), F32), pltpu.VMEM((64, 128), F32), pltpu.VMEM((128, 128), F32),
            pltpu.VMEM((2, 3, rows // 2, 128), F32), pltpu.VMEM((2, 3, rows, 128), F32),
            pltpu.VMEM((2, 3, rows // 2, 128), F32),
            pltpu.SemaphoreType.DMA((3,)), pltpu.SemaphoreType.DMA((22,)), pltpu.SemaphoreType.DMA((22,)),
        ],
        compiler_params=pltpu.CompilerParams(collective_id=2, has_side_effects=True, vmem_limit_bytes=60 * 1024 * 1024),
        name="solve_points",
    )(reduced, cameras, increment, points, gradient, inverse)
    return new, table.reshape(nx * ny * nc * nz * CT, 128)


def rows_of(x):
    n = x.shape[1] // 128
    return x.reshape(x.shape[0], n, 128).transpose(1, 0, 2).reshape(n * x.shape[0], 128)


def on_device(cameras, increment, points, gradient, inverse, cj, pj, observed, tb, tp, oc, op, accept):
    oc2 = oc.reshape(-1, 128)
    op2 = op.reshape(-1, 128)
    reduced, kept = reduce_points(gather_rows(increment), cj, pj, oc2, op2, tb, tp, accept.reshape(1), cameras, increment, points.shape[1])
    new, table = solve_points(reduced, cameras, increment, points, gradient, inverse)
    res, cost = project_points(table, new.reshape(-1, 128), oc2, op2, rows_of(observed), tb, tp)
    n = observed.shape[1]
    residual = res.reshape(n // 128, 2, 128).transpose(1, 0, 2).reshape(2, n)
    total = total_cost(cost, 1.0 / (2.0 * n * lax.axis_size(PTS_CAM)))
    accepted = jnp.where((accept & 1) == 1, new.reshape(3, -1), points)
    return residual, total, accepted, kept


def solution(mesh):
    split = Mesh(mesh.devices.reshape(4, 4, 2, mesh.shape["cam"]), PTS_CAM)
    in_specs = (P(None, PTS_CAM), P(None, PTS_CAM), P(None, PTS), P(None, PTS), P(None, PTS),
                P(None, PTS_CAM), P(None, PTS_CAM), P(None, PTS_CAM),
                P(PTS_CAM), P(PTS_CAM), P(PTS_CAM), P(PTS_CAM), P())
    out_specs = (P(None, PTS_CAM), P(), P(None, PTS), P(None, PTS_CAM))
    return jax.shard_map(on_device, mesh=split, in_specs=in_specs, out_specs=out_specs, check_vma=False)
```

```python
import functools, math
import jax, jax.numpy as jnp
from jax import lax
from jax.experimental import pallas as pl
from jax.experimental.pallas import tpu as pltpu
from jax.sharding import Mesh
from jax.sharding import PartitionSpec as P

CB=128; PB=256; TILE=256
F32=jnp.float32
GROUP=1024
TPG=GROUP//TILE

def lane_gather(table, index):
    return lax.gather(table, index[..., None],
        lax.GatherDimensionNumbers(offset_dims=(), collapsed_slice_dims=(1,), start_index_map=(1,),
            operand_batching_dims=(0,), start_indices_batching_dims=(0,)),
        slice_sizes=(1,1), mode=lax.GatherScatterMode.PROMISE_IN_BOUNDS)

def tile_rows(rows, row_id):
    a,b,c,d = rows
    return jnp.where(row_id<4, jnp.where(row_id<2,a,b), jnp.where(row_id<6,c,d))

def spread(ref, first):
    return ref[pl.ds(first, 8, stride=0), :]

PH=8; PL=32
UN=16

def reduce_body(chunk, blocks_n, tb, tp, word, inc_ref, cj_ref, pj_ref, oc_ref, op_ref, cam_ref, own_ref, out_ref, kept_ref, acc, jscr, pscr, wscr):
    step = pl.program_id(0)
    groups = chunk//GROUP
    row_id = lax.broadcasted_iota(jnp.int32,(8,128),0)
    @pl.when(step==0)
    def _():
        def zero(i,_):
            acc[pl.ds(pl.multiple_of(i*(PH*8),PH*8),PH*8),:] = jnp.zeros((PH*8,PL),F32)
            return 0
        lax.fori_loop(0, blocks_n, zero, 0, unroll=8)
        wscr[...] = jnp.zeros_like(wscr)
        kept_ref[...] = cam_ref[...] + (word[0] & 1).astype(F32)*own_ref[...]
    def couple(g, slot):
        base = step*(chunk//TILE) + g*TPG
        cams = [tb[base+i]*9 for i in range(TPG)]
        cam = oc_ref[pl.ds(pl.multiple_of(g*8,8),8),:]
        for j in range(8):
            at = pl.ds(pl.multiple_of(g*GROUP+j*128,128),128)
            jscr[slot, j*24:j*24+18,:] = cj_ref[:,at].astype(F32)
            pscr[slot, j*8:j*8+6,:] = pj_ref[:,at].astype(F32)
        first=second=None
        for m in range(9):
            t = tile_rows([spread(inc_ref, c+m) for c in cams], row_id)
            v = lane_gather(t, cam)
            a = jscr[slot, pl.ds(m,8,stride=24),:]*v
            b = jscr[slot, pl.ds(9+m,8,stride=24),:]*v
            first = a if first is None else first+a
            second = b if second is None else second+b
        for n in range(3):
            v = pscr[slot, pl.ds(n,8,stride=8),:]*first + pscr[slot, pl.ds(3+n,8,stride=8),:]*second
            hi = v.astype(jnp.bfloat16).astype(F32)
            wscr[slot, pl.ds(n,8,stride=8),:] = hi
            wscr[slot, pl.ds(3+n,8,stride=8),:] = v-hi
    def scatter(g, slot):
        base = step*(chunk//TILE) + g*TPG
        for t in range(TPG):
            lhs=[]; rhs=[]
            for h in range(2):
                s=2*t+h
                w = wscr[slot, s*8:s*8+8,:]
                ids = op_ref[pl.ds(g*8+s,8,stride=0),:]
                hi = lax.shift_right_logical(ids,PL.bit_length()-1)
                lo = ids & (PL-1)
                lhs.append(jnp.concatenate([jnp.where(hi==k,w,0.0) for k in range(PH)],axis=0).astype(jnp.bfloat16))
                rhs.append(jnp.concatenate([jnp.where(lo-8*k==row_id,1.0,0.0) for k in range(PL//8)],axis=0).astype(jnp.bfloat16))
            L=jnp.concatenate(lhs,axis=1); R=jnp.concatenate(rhs,axis=1)
            r = lax.dot_general(L,R,(((1,),(1,)),((),())),preferred_element_type=F32)
            at = pl.ds(pl.multiple_of(tp[base+t]*(PH*8),PH*8),PH*8)
            acc[at,:] += r
    def body(i,_):
        for u in range(UN): couple(i*UN+u, u)
        for u in range(UN): scatter(i*UN+u, u)
        return 0
    lax.fori_loop(0, groups//UN, body, 0)
    @pl.when(step==pl.num_programs(0)-1)
    def _():
        def flush(i,_):
            for h in range(2):
                n = 128//PL
                x = jnp.concatenate([acc[pl.ds(pl.multiple_of(i*(PH*8)+(h*n+k)*8,8),8),:] for k in range(n)],axis=1)
                s = x[0:3,:]+x[3:6,:]
                for n in range(3):
                    out_ref[n, pl.ds(2*i+h,1),:] = s[n:n+1,:]
            return 0
        lax.fori_loop(0, blocks_n, flush, 0, unroll=32)

def reduce_points(inc, cj, pj, oc, op, tb, tp, word, cameras, increment, npts, chunk=16384):
    n=cj.shape[1]
    blocks_n=npts//PB
    return pl.pallas_call(
        functools.partial(reduce_body, chunk, blocks_n),
        out_shape=(jax.ShapeDtypeStruct((3,npts//128,128),F32), jax.ShapeDtypeStruct((9,128),F32)),
        grid_spec=pltpu.PrefetchScalarGridSpec(
            num_scalar_prefetch=3, grid=(n//chunk,),
            in_specs=[
                pl.BlockSpec(inc.shape, lambda i,*_:(0,0)),
                pl.BlockSpec((18,chunk), lambda i,*_:(0,i)),
                pl.BlockSpec((6,chunk), lambda i,*_:(0,i)),
                pl.BlockSpec((chunk//128,128), lambda i,*_:(i,0)),
                pl.BlockSpec((chunk//128,128), lambda i,*_:(i,0)),
                pl.BlockSpec((9,128), lambda i,*_:(0,0)),
                pl.BlockSpec((9,128), lambda i,*_:(0,0)),
            ],
            out_specs=(pl.BlockSpec((3,npts//128,128), lambda i,*_:(0,0,0)), pl.BlockSpec((9,128), lambda i,*_:(0,0))),
            scratch_shapes=[pltpu.VMEM((blocks_n*PH*8,PL),F32), pltpu.VMEM((UN,192,128),F32), pltpu.VMEM((UN,64,128),F32), pltpu.VMEM((UN,64,128),F32)],
        ),
        cost_estimate=pl.CostEstimate(flops=10000000000, bytes_accessed=1000000, transcendentals=0),
        compiler_params=pltpu.CompilerParams(dimension_semantics=("arbitrary",), vmem_limit_bytes=28*1024*1024),
        name="reduce_points",
    )(tb,tp,word,inc,cj,pj,oc,op,cameras,increment)

CT=10
def project_body(chunk, tb, tp, cam_ref, pts_ref, oc_ref, op_ref, ob_ref, res_ref, cost_ref):
    step=pl.program_id(0)
    groups=chunk//GROUP
    row_id=lax.broadcasted_iota(jnp.int32,(8,128),0)
    @pl.when(step==0)
    def _():
        cost_ref[...]=jnp.zeros_like(cost_ref)
    def one(g):
        base=step*(chunk//TILE)+g*TPG
        cams=[tb[base+i]*CT for i in range(TPG)]
        pts=[tp[base+i]*2 for i in range(TPG)]
        at8=pl.ds(pl.multiple_of(g*8,8),8)
        cam=oc_ref[at8,:]; pid=op_ref[at8,:]
        half=pts_ref.shape[0]//3
        upper=pid>=128; plow=pid&127
        def look(r): return lane_gather(tile_rows([spread(cam_ref,c+r) for c in cams],row_id),cam)
        def lookp(r):
            a=lane_gather(tile_rows([spread(pts_ref,p+r*half) for p in pts],row_id),plow)
            b=lane_gather(tile_rows([spread(pts_ref,p+r*half+1) for p in pts],row_id),plow)
            return jnp.where(upper,b,a)
        x,y,z=lookp(0),lookp(1),lookp(2)
        vx,vy,vz,r,t0,t1,t2,f0,f1,f2=[look(i) for i in range(CT)]
        ax=vy*z-vz*y; ay=vz*x-vx*z; az=vx*y-vy*x
        px=x+r*ax+(vy*az-vz*ay)+t0
        py=y+r*ay+(vz*ax-vx*az)+t1
        pz=z+r*az+(vx*ay-vy*ax)+t2
        inv=1.0/jnp.maximum(-pz,1.0)
        u=px*inv; v=py*inv
        q=u*u+v*v
        fac=f0+q*(f1+q*f2)
        o0=pl.ds(g*16,8,stride=2); o1=pl.ds(g*16+1,8,stride=2)
        ru=fac*u-ob_ref[o0,:]; rv=fac*v-ob_ref[o1,:]
        res_ref[o0,:]=ru; res_ref[o1,:]=rv
        return ru*ru+rv*rv
    def body(i,c):
        for u in range(16): c=c+one(i*16+u)
        return c
    cost_ref[...]+=lax.fori_loop(0,groups//16,body,jnp.zeros((8,128),F32))

def project_points(cam, pts, oc, op, ob, tb, tp, chunk=65536):
    n=oc.shape[0]*128
    return pl.pallas_call(
        functools.partial(project_body, chunk),
        out_shape=(jax.ShapeDtypeStruct((n//64,128),F32), jax.ShapeDtypeStruct((8,128),F32)),
        grid_spec=pltpu.PrefetchScalarGridSpec(
            num_scalar_prefetch=2, grid=(n//chunk,),
            in_specs=[
                pl.BlockSpec(cam.shape, lambda i,*_:(0,0)),
                pl.BlockSpec(pts.shape, lambda i,*_:(0,0)),
                pl.BlockSpec((chunk//128,128), lambda i,*_:(i,0)),
                pl.BlockSpec((chunk//128,128), lambda i,*_:(i,0)),
                pl.BlockSpec((chunk//64,128), lambda i,*_:(i,0)),
            ],
            out_specs=(pl.BlockSpec((chunk//64,128), lambda i,*_:(i,0)), pl.BlockSpec((8,128), lambda i,*_:(0,0))),
        ),
        cost_estimate=pl.CostEstimate(flops=5000000000, bytes_accessed=1000000, transcendentals=0),
        compiler_params=pltpu.CompilerParams(dimension_semantics=("arbitrary",), vmem_limit_bytes=20*1024*1024),
        name="project_points",
    )(tb,tp,cam,pts,oc,op,ob)


MESH = pl.DeviceIdType.MESH
X, Y, CORE, CAM = "pts_0", "pts_1", "pts_2", "cam"
PTS = (X, Y, CORE)
PTS_CAM = PTS + (CAM,)


def peer(axis, hop):
    n = lax.axis_size(axis)
    return {axis: lax.rem(lax.axis_index(axis) + hop, n)}


def greet(peers):
    barrier = pltpu.get_barrier_semaphore()
    for p in peers:
        pl.semaphore_signal(barrier, inc=1, device_id=p, device_id_type=MESH)
    pl.semaphore_wait(barrier, len(peers))


def hops(axis):
    return range(1, lax.axis_size(axis))


def send(src, dst, send_sem, recv_sem, to):
    copy = pltpu.make_async_remote_copy(src, dst, send_sem, recv_sem, device_id=to, device_id_type=MESH)
    copy.start()
    return copy


def gather_body(local_ref, out_ref, send_sem, recv_sem):
    at = {a: lax.axis_index(a) for a in (X, Y, CORE, CAM)}

    def part(k, whole):
        i = [slice(None) if a in whole else at[a] for a in (X, Y, CORE, CAM)]
        return out_ref.at[(*i, pl.ds(3 * k, 3))]

    for i in range(9):
        out_ref[at[X], at[Y], at[CORE], at[CAM], i] = local_ref[i:i + 1, :]
    greet([peer(a, h) for a in (CAM, Y, X, CORE) for h in hops(a)])
    order = ((CAM, Y, X), (Y, X, CAM), (X, CAM, Y))
    def start(k, stage):
        axis, done = order[k][stage], order[k][:stage]
        first = 9 * k + 3 * stage
        return [send(part(k, done), part(k, done), send_sem.at[first + h - 1], recv_sem.at[first + h - 1], peer(axis, h))
                for h in hops(axis)]

    sent = []
    flying = [start(k, 0) for k in range(3)]
    for stage in range(1, 4):
        for k in range(3):
            for cp in flying[k]:
                cp.wait_recv()
            sent += flying[k]
            if stage < 3:
                flying[k] = start(k, stage)
    half = out_ref.at[:, :, at[CORE]]
    last = send(half, half, send_sem.at[27], recv_sem.at[27], peer(CORE, 1))
    for cp in sent:
        cp.wait_send()
    last.wait()


def gather_rows(local):
    rows = local.shape[0]
    nx, ny, nc, nz = [lax.axis_size(a) for a in (X, Y, CORE, CAM)]
    out = pl.pallas_call(
        gather_body,
        out_shape=jax.ShapeDtypeStruct((nx, ny, nc, nz, rows, 1, 128), F32),
        in_specs=[pl.BlockSpec(memory_space=pltpu.VMEM)],
        out_specs=pl.BlockSpec(memory_space=pltpu.VMEM),
        scratch_shapes=[pltpu.SemaphoreType.DMA((28,)), pltpu.SemaphoreType.DMA((28,))],
        cost_estimate=pl.CostEstimate(flops=20000000000, bytes_accessed=1000000, transcendentals=0),
        compiler_params=pltpu.CompilerParams(collective_id=0, has_side_effects=True, vmem_limit_bytes=8*1024*1024),
        name="gather_rows",
    )(local)
    return out.reshape(nx * ny * nc * nz * rows, 128)


def cost_peers():
    near = [{**peer(Y, i), **peer(CAM, j)} for i in range(4) for j in range(4) if i or j]
    far = [{**peer(X, i), **peer(CORE, j)} for i in range(4) for j in range(2) if i or j]
    return near, far


def cost_body(scale, part_ref, out_ref, buf, send_sem, recv_sem):
    x, y, c, z = [lax.axis_index(a) for a in (X, Y, CORE, CAM)]
    peers = cost_peers()
    greet(peers[0] + peers[1])
    value = part_ref[...]
    slot = 0
    for stage, (me, count) in enumerate(((y * 4 + z, 16), (x * 2 + c, 8))):
        buf[stage, pl.ds(pl.multiple_of(me * 8, 8), 8), :] = value
        own = buf.at[stage, pl.ds(pl.multiple_of(me * 8, 8), 8)]
        copies = []
        for p in peers[stage]:
            copies.append(send(own, own, send_sem.at[slot], recv_sem.at[slot], p))
            slot += 1
        for cp in copies:
            cp.wait()
        value = buf[stage, 0:8, :]
        for k in range(1, count):
            value = value + buf[stage, k * 8:k * 8 + 8, :]
    out_ref[...] = jnp.sum(value, axis=(0, 1), keepdims=True) * scale


def total_cost(part, scale):
    out = pl.pallas_call(
        functools.partial(cost_body, scale),
        out_shape=jax.ShapeDtypeStruct((1, 1), F32),
        in_specs=[pl.BlockSpec(memory_space=pltpu.VMEM)],
        out_specs=pl.BlockSpec(memory_space=pltpu.VMEM),
        scratch_shapes=[pltpu.VMEM((2, 128, 128), F32), pltpu.SemaphoreType.DMA((22,)), pltpu.SemaphoreType.DMA((22,))],
        cost_estimate=pl.CostEstimate(flops=5000000000, bytes_accessed=1000000, transcendentals=0),
        compiler_params=pltpu.CompilerParams(collective_id=1, has_side_effects=True, vmem_limit_bytes=4*1024*1024),
        name="total_cost",
    )(part)
    return out.reshape(())


RT2 = math.sqrt(2.0)


def camera_rows(trial):
    w = [trial[i:i + 1] for i in range(3)]
    half = 0.5 * jnp.sqrt(w[0] * w[0] + w[1] * w[1] + w[2] * w[2])
    zero = half == 0.0
    ratio = (0.5 * RT2) * jnp.where(zero, 1.0, jnp.sin(half) / jnp.where(zero, 1.0, half))
    f = trial[6:7]
    return [ratio * a for a in w] + [RT2 * jnp.cos(half), trial[3:4], trial[4:5], trial[5:6], f, f * trial[7:8], f * trial[8:9]]


def solve_body(red_ref, cam_ref, inc_ref, pts_hbm, grad_hbm, inv_hbm, new_ref, tab_ref, pts, grad, inv, pscr, gscr, iscr,
               far, near, total, local_sem, send_sem, recv_sem):
    cx, cy, cc = [lax.axis_index(a) for a in (X, Y, CORE)]
    z = lax.axis_index(CAM)
    n = lax.axis_size(CAM)
    rows = red_ref.shape[1] // n
    half = rows // 2
    lanes = pl.ds(pl.multiple_of(z * (rows * 128), 128), rows * 128)
    loads = [pltpu.make_async_copy(src.at[:, lanes], dst, local_sem.at[i])
             for i, (src, dst) in enumerate(((pts_hbm, pts), (grad_hbm, grad), (inv_hbm, inv)))]
    for cp in loads:
        cp.start()
    right, left = peer(CAM, 1), peer(CAM, n - 1)
    for i, row in enumerate(camera_rows(cam_ref[...] + inc_ref[...])):
        tab_ref[cx, cy, cc, z, i] = row
    greet([peer(a, h) for a in (CAM, Y, X, CORE) for h in hops(a)])

    def spread_table(axis, part, slot):
        return [send(part, part, send_sem.at[slot + h - 1], recv_sem.at[slot + h - 1], peer(axis, h)) for h in hops(axis)]

    table = spread_table(CAM, tab_ref.at[cx, cy, cc, z], 10)

    def at(k):
        return lax.rem(z + k, n) * rows

    a = send(red_ref.at[:, pl.ds(at(2), half)], far.at[0], send_sem.at[0], recv_sem.at[0], right)
    b = send(red_ref.at[:, pl.ds(at(2) + half, half)], far.at[1], send_sem.at[1], recv_sem.at[1], left)
    c = send(red_ref.at[:, pl.ds(at(1) + half, half)], near.at[0, :, pl.ds(half, half)], send_sem.at[2], recv_sem.at[2], right)
    d = send(red_ref.at[:, pl.ds(at(n - 1), half)], near.at[1, :, pl.ds(0, half)], send_sem.at[3], recv_sem.at[3], left)
    a.wait_recv()
    total[0] = red_ref[:, pl.ds(at(1), half), :] + far[0]
    e = send(total.at[0], near.at[0, :, pl.ds(0, half)], send_sem.at[4], recv_sem.at[4], right)
    b.wait_recv()
    total[1] = red_ref[:, pl.ds(at(n - 1) + half, half), :] + far[1]
    f = send(total.at[1], near.at[1, :, pl.ds(half, half)], send_sem.at[5], recv_sem.at[5], left)
    for cp in table:
        cp.wait()
    table = spread_table(Y, tab_ref.at[cx, cy, cc], 13)
    for cp in loads:
        cp.wait()
    c.wait_recv()
    d.wait_recv()
    e.wait_recv()
    f.wait_recv()

    def group(g, _):
        r8 = pl.ds(pl.multiple_of(g * 8, 8), 8)
        for j in range(8):
            l = pl.ds(pl.multiple_of(g * 1024 + j * 128, 128), 128)
            pscr[pl.ds(j * 8, 3), :] = pts[:, l]
            gscr[pl.ds(j * 8, 3), :] = grad[:, l]
            iscr[pl.ds(j * 16, 9), :] = inv[:, l]
        own = pl.ds(pl.multiple_of(z * rows + g * 8, 8), 8)
        res = [gscr[pl.ds(k, 8, stride=8), :]
               - (red_ref[k, own, :] + near[0, k, r8, :] + near[1, k, r8, :]) for k in range(3)]
        for i in range(3):
            step = (iscr[pl.ds(3 * i, 8, stride=16), :] * res[0] + iscr[pl.ds(3 * i + 1, 8, stride=16), :] * res[1]
                    + iscr[pl.ds(3 * i + 2, 8, stride=16), :] * res[2])
            new_ref[i, own, :] = pscr[pl.ds(i, 8, stride=8), :] + step
        return 0

    def own(part):
        return new_ref.at[:, pl.ds(z * rows + part * half, half)]

    lax.fori_loop(0, half // 8, group, 0)
    g = send(own(0), own(0), send_sem.at[6], recv_sem.at[6], right)
    lax.fori_loop(half // 8, rows // 8, group, 0)
    h = send(own(1), own(1), send_sem.at[7], recv_sem.at[7], left)
    g2 = send(own(1), own(1), send_sem.at[8], recv_sem.at[8], right)
    h2 = send(own(0), own(0), send_sem.at[9], recv_sem.at[9], left)
    for cp in table:
        cp.wait()
    table = spread_table(X, tab_ref.at[cx, :, cc], 16)
    g.wait_recv()
    first = new_ref.at[:, pl.ds(at(n - 1), half)]
    k = send(first, first, send_sem.at[20], recv_sem.at[20], right)
    h.wait_recv()
    second = new_ref.at[:, pl.ds(at(1) + half, half)]
    m = send(second, second, send_sem.at[21], recv_sem.at[21], left)
    for cp in table:
        cp.wait()
    table = spread_table(CORE, tab_ref.at[:, :, cc], 19)
    for cp in (g2, h2, k, m):
        cp.wait_recv()
    for cp in (a, b, c, d, e, f, g, h, g2, h2, k, m):
        cp.wait_send()
    for cp in table:
        cp.wait()


def solve_points(reduced, cameras, increment, points, gradient, inverse):
    rows = reduced.shape[1] // 4
    nx, ny, nc, nz = [lax.axis_size(a) for a in (X, Y, CORE, CAM)]
    hbm = pl.BlockSpec(memory_space=pl.ANY)
    vmem = pl.BlockSpec(memory_space=pltpu.VMEM)
    new, table = pl.pallas_call(
        solve_body,
        out_shape=(jax.ShapeDtypeStruct(reduced.shape, F32), jax.ShapeDtypeStruct((nx, ny, nc, nz, CT, 1, 128), F32)),
        in_specs=[vmem, vmem, vmem, hbm, hbm, hbm],
        out_specs=(vmem, vmem),
        scratch_shapes=[
            pltpu.VMEM((3, rows * 128), F32), pltpu.VMEM((3, rows * 128), F32), pltpu.VMEM((9, rows * 128), F32),
            pltpu.VMEM((64, 128), F32), pltpu.VMEM((64, 128), F32), pltpu.VMEM((128, 128), F32),
            pltpu.VMEM((2, 3, rows // 2, 128), F32), pltpu.VMEM((2, 3, rows, 128), F32),
            pltpu.VMEM((2, 3, rows // 2, 128), F32),
            pltpu.SemaphoreType.DMA((3,)), pltpu.SemaphoreType.DMA((22,)), pltpu.SemaphoreType.DMA((22,)),
        ],
        cost_estimate=pl.CostEstimate(flops=8000000000, bytes_accessed=1000000, transcendentals=0),
        compiler_params=pltpu.CompilerParams(collective_id=2, has_side_effects=True, vmem_limit_bytes=16*1024*1024),
        name="solve_points",
    )(reduced, cameras, increment, points, gradient, inverse)
    return new, table.reshape(nx * ny * nc * nz * CT, 128)


def rows_of(x):
    n = x.shape[1] // 128
    return x.reshape(x.shape[0], n, 128).transpose(1, 0, 2).reshape(n * x.shape[0], 128)


def on_device(cameras, increment, points, gradient, inverse, cj, pj, observed, tb, tp, oc, op, accept):
    oc2 = oc.reshape(-1, 128)
    op2 = op.reshape(-1, 128)
    reduced, kept = reduce_points(gather_rows(increment), cj, pj, oc2, op2, tb, tp, accept.reshape(1), cameras, increment, points.shape[1])
    new, table = solve_points(reduced, cameras, increment, points, gradient, inverse)
    res, cost = project_points(table, new.reshape(-1, 128), oc2, op2, rows_of(observed), tb, tp)
    n = observed.shape[1]
    residual = res.reshape(n // 128, 2, 128).transpose(1, 0, 2).reshape(2, n)
    total = total_cost(cost, 1.0 / (2.0 * n * lax.axis_size(PTS_CAM)))
    accepted = jnp.where((accept & 1) == 1, new.reshape(3, -1), points)
    return residual, total, accepted, kept


def solution(mesh):
    split = Mesh(mesh.devices.reshape(4, 4, 2, mesh.shape["cam"]), PTS_CAM)
    in_specs = (P(None, PTS_CAM), P(None, PTS_CAM), P(None, PTS), P(None, PTS), P(None, PTS),
                P(None, PTS_CAM), P(None, PTS_CAM), P(None, PTS_CAM),
                P(PTS_CAM), P(PTS_CAM), P(PTS_CAM), P(PTS_CAM), P())
    out_specs = (P(None, PTS_CAM), P(), P(None, PTS), P(None, PTS_CAM))
    return jax.shard_map(on_device, mesh=split, in_specs=in_specs, out_specs=out_specs, check_vma=False)
```

```python
import functools, math
import jax, jax.numpy as jnp
from jax import lax
from jax.experimental import pallas as pl
from jax.experimental.pallas import tpu as pltpu
from jax.sharding import Mesh
from jax.sharding import PartitionSpec as P

CB=128; PB=256; TILE=256
F32=jnp.float32
GROUP=1024
TPG=GROUP//TILE

def lane_gather(table, index):
    return lax.gather(table, index[..., None],
        lax.GatherDimensionNumbers(offset_dims=(), collapsed_slice_dims=(1,), start_index_map=(1,),
            operand_batching_dims=(0,), start_indices_batching_dims=(0,)),
        slice_sizes=(1,1), mode=lax.GatherScatterMode.PROMISE_IN_BOUNDS)

def tile_rows(rows, row_id):
    a,b,c,d = rows
    return jnp.where(row_id<4, jnp.where(row_id<2,a,b), jnp.where(row_id<6,c,d))

def spread(ref, first):
    return ref[pl.ds(first, 8, stride=0), :]

PH=8; PL=32
UN=32

def reduce_body(chunk, blocks_n, tb, tp, word, inc_ref, cj_ref, pj_ref, oc_ref, op_ref, cam_ref, own_ref, out_ref, kept_ref, acc, jscr, pscr, wscr):
    step = 0
    groups = oc_ref.shape[0]//8
    row_id = lax.broadcasted_iota(jnp.int32,(8,128),0)
    if True:
        def zero(i,_):
            acc[pl.ds(pl.multiple_of(i*(PH*8),PH*8),PH*8),:] = jnp.zeros((PH*8,PL),F32)
            return 0
        lax.fori_loop(0, blocks_n, zero, 0, unroll=8)
        wscr[...] = jnp.zeros_like(wscr)
        kept_ref[...] = cam_ref[...] + (word[0] & 1).astype(F32)*own_ref[...]
    def couple(g, slot):
        base = step*(chunk//TILE) + g*TPG
        cams = [tb[base+i]*9 for i in range(TPG)]
        cam = oc_ref[pl.ds(pl.multiple_of(g*8,8),8),:]
        for j in range(8):
            at = pl.ds(pl.multiple_of(g*GROUP+j*128,128),128)
            jscr[slot, j*24:j*24+18,:] = cj_ref[:,at].astype(F32)
            pscr[slot, j*8:j*8+6,:] = pj_ref[:,at].astype(F32)
        first=second=None
        for m in range(9):
            t = tile_rows([spread(inc_ref, c+m) for c in cams], row_id)
            v = lane_gather(t, cam)
            a = jscr[slot, pl.ds(m,8,stride=24),:]*v
            b = jscr[slot, pl.ds(9+m,8,stride=24),:]*v
            first = a if first is None else first+a
            second = b if second is None else second+b
        for n in range(3):
            v = pscr[slot, pl.ds(n,8,stride=8),:]*first + pscr[slot, pl.ds(3+n,8,stride=8),:]*second
            hi = v.astype(jnp.bfloat16).astype(F32)
            wscr[slot, pl.ds(n,8,stride=8),:] = hi
            wscr[slot, pl.ds(3+n,8,stride=8),:] = v-hi
    def scatter(g, slot):
        base = step*(chunk//TILE) + g*TPG
        for t in range(TPG):
            lhs=[]; rhs=[]
            for h in range(2):
                s=2*t+h
                w = wscr[slot, s*8:s*8+8,:]
                ids = op_ref[pl.ds(g*8+s,8,stride=0),:]
                hi = lax.shift_right_logical(ids,PL.bit_length()-1)
                lo = ids & (PL-1)
                lhs.append(jnp.concatenate([jnp.where(hi==k,w,0.0) for k in range(PH)],axis=0).astype(jnp.bfloat16))
                rhs.append(jnp.concatenate([jnp.where(lo-8*k==row_id,1.0,0.0) for k in range(PL//8)],axis=0).astype(jnp.bfloat16))
            L=jnp.concatenate(lhs,axis=1); R=jnp.concatenate(rhs,axis=1)
            r = lax.dot_general(L,R,(((1,),(1,)),((),())),preferred_element_type=F32)
            at = pl.ds(pl.multiple_of(tp[base+t]*(PH*8),PH*8),PH*8)
            acc[at,:] += r
    def body(i,_):
        for u in range(UN): couple(i*UN+u, u)
        for u in range(UN): scatter(i*UN+u, u)
        return 0
    lax.fori_loop(0, groups//UN, body, 0)
    if True:
        def flush(i,_):
            for h in range(2):
                n = 128//PL
                x = jnp.concatenate([acc[pl.ds(pl.multiple_of(i*(PH*8)+(h*n+k)*8,8),8),:] for k in range(n)],axis=1)
                s = x[0:3,:]+x[3:6,:]
                for n in range(3):
                    out_ref[n, pl.ds(2*i+h,1),:] = s[n:n+1,:]
            return 0
        lax.fori_loop(0, blocks_n, flush, 0, unroll=32)

def reduce_points(inc, cj, pj, oc, op, tb, tp, word, cameras, increment, npts, chunk=16384):
    n=cj.shape[1]
    blocks_n=npts//PB
    return pl.pallas_call(
        functools.partial(reduce_body, chunk, blocks_n),
        out_shape=(jax.ShapeDtypeStruct((3,npts//128,128),F32), jax.ShapeDtypeStruct((9,128),F32)),
        in_specs=[pl.BlockSpec(memory_space=pltpu.SMEM)]*3+[pl.BlockSpec(memory_space=pltpu.VMEM)]*7,
        out_specs=(pl.BlockSpec(memory_space=pltpu.VMEM), pl.BlockSpec(memory_space=pltpu.VMEM)),
            scratch_shapes=[pltpu.VMEM((blocks_n*PH*8,PL),F32), pltpu.VMEM((UN,192,128),F32), pltpu.VMEM((UN,64,128),F32), pltpu.VMEM((UN,64,128),F32)],
        cost_estimate=pl.CostEstimate(flops=10000000000, bytes_accessed=1000000, transcendentals=0),
        compiler_params=pltpu.CompilerParams(vmem_limit_bytes=28*1024*1024),
        name="reduce_points",
    )(tb,tp,word,inc,cj,pj,oc,op,cameras,increment)

CT=10
TURN=16

def project_body(tb, tp, word, cam_ref, pts_ref, oc_ref, op_ref, ob_ref, old_ref, res_hbm, acc_hbm, cost_ref, res_ref, acc_ref, sem):
    turns=oc_ref.shape[0]//(8*TURN)
    spans=old_ref.shape[1]//(128*turns)
    row_id=lax.broadcasted_iota(jnp.int32,(8,128),0)
    taken=jnp.broadcast_to(word[0]&1,(3,128))==1
    def one(g):
        base=g*TPG
        cams=[tb[base+i]*CT for i in range(TPG)]
        pts=[tp[base+i]*2 for i in range(TPG)]
        at8=pl.ds(pl.multiple_of(g*8,8),8)
        cam=oc_ref[at8,:]; pid=op_ref[at8,:]
        half=pts_ref.shape[0]//3
        upper=pid>=128; plow=pid&127
        def look(r): return lane_gather(tile_rows([spread(cam_ref,c+r) for c in cams],row_id),cam)
        def lookp(r):
            a=lane_gather(tile_rows([spread(pts_ref,p+r*half) for p in pts],row_id),plow)
            b=lane_gather(tile_rows([spread(pts_ref,p+r*half+1) for p in pts],row_id),plow)
            return jnp.where(upper,b,a)
        x,y,z=lookp(0),lookp(1),lookp(2)
        vx,vy,vz,r,t0,t1,t2,f0,f1,f2=[look(i) for i in range(CT)]
        ax=vy*z-vz*y; ay=vz*x-vx*z; az=vx*y-vy*x
        px=x+r*ax+(vy*az-vz*ay)+t0
        py=y+r*ay+(vz*ax-vx*az)+t1
        pz=z+r*az+(vx*ay-vy*ax)+t2
        inv=1.0/jnp.maximum(-pz,1.0)
        u=px*inv; v=py*inv
        q=u*u+v*v
        fac=f0+q*(f1+q*f2)
        o0=pl.ds(g*16,8,stride=2); o1=pl.ds(g*16+1,8,stride=2)
        ru=fac*u-ob_ref[o0,:]; rv=fac*v-ob_ref[o1,:]
        res_ref[o0,:]=ru; res_ref[o1,:]=rv
        return ru*ru+rv*rv
    def out(i):
        rows=pl.ds(pl.multiple_of(i*(TURN*16),TURN*16),TURN*16)
        lanes=pl.ds(pl.multiple_of(i*(spans*128),spans*128),spans*128)
        return (pltpu.make_async_copy(res_ref.at[rows],res_hbm.at[rows],sem.at[0,i]),
                pltpu.make_async_copy(acc_ref.at[:,lanes],acc_hbm.at[:,lanes],sem.at[1,i]))
    def body(i,c):
        for u in range(TURN): c=c+one(i*TURN+u)
        for j in range(spans):
            row=i*spans+j
            lanes=pl.ds(pl.multiple_of(row*128,128),128)
            new=jnp.concatenate([pts_ref[pl.ds(row+k*(spans*turns),1),:] for k in range(3)],axis=0)
            acc_ref[:,lanes]=jnp.where(taken,new,old_ref[:,lanes])
        for cp in out(i): cp.start()
        return c
    cost_ref[...]=lax.fori_loop(0,turns,body,jnp.zeros((8,128),F32))
    def finish(i,_):
        for cp in out(i): cp.wait()
        return 0
    lax.fori_loop(0,turns,finish,0)

def project_points(cam, pts, oc, op, ob, tb, tp, word, old):
    n=oc.shape[0]*128
    turns=n//(GROUP*TURN)
    smem=pl.BlockSpec(memory_space=pltpu.SMEM)
    vmem=pl.BlockSpec(memory_space=pltpu.VMEM)
    hbm=pl.BlockSpec(memory_space=pl.ANY)
    return pl.pallas_call(
        project_body,
        out_shape=(jax.ShapeDtypeStruct((n//64,128),F32), jax.ShapeDtypeStruct(old.shape,F32), jax.ShapeDtypeStruct((8,128),F32)),
        in_specs=[smem]*3+[vmem]*6,
        out_specs=(hbm,hbm,vmem),
        scratch_shapes=[pltpu.VMEM((n//64,128),F32), pltpu.VMEM(old.shape,F32), pltpu.SemaphoreType.DMA((2,turns))],
        cost_estimate=pl.CostEstimate(flops=5000000000, bytes_accessed=1000000, transcendentals=0),
        compiler_params=pltpu.CompilerParams(vmem_limit_bytes=20*1024*1024),
        name="project_points",
    )(tb,tp,word,cam,pts,oc,op,ob,old)


MESH = pl.DeviceIdType.MESH
X, Y, CORE, CAM = "pts_0", "pts_1", "pts_2", "cam"
PTS = (X, Y, CORE)
PTS_CAM = PTS + (CAM,)


def peer(axis, hop):
    n = lax.axis_size(axis)
    return {axis: lax.rem(lax.axis_index(axis) + hop, n)}


def greet(peers):
    barrier = pltpu.get_barrier_semaphore()
    for p in peers:
        pl.semaphore_signal(barrier, inc=1, device_id=p, device_id_type=MESH)
    pl.semaphore_wait(barrier, len(peers))


def hops(axis):
    return range(1, lax.axis_size(axis))


def send(src, dst, send_sem, recv_sem, to):
    copy = pltpu.make_async_remote_copy(src, dst, send_sem, recv_sem, device_id=to, device_id_type=MESH)
    copy.start()
    return copy


def gather_body(local_ref, out_ref, send_sem, recv_sem):
    at = {a: lax.axis_index(a) for a in (X, Y, CORE, CAM)}

    def part(k, whole):
        i = [slice(None) if a in whole else at[a] for a in (X, Y, CORE, CAM)]
        return out_ref.at[(*i, pl.ds(3 * k, 3))]

    for i in range(9):
        out_ref[at[X], at[Y], at[CORE], at[CAM], i] = local_ref[i:i + 1, :]
    greet([peer(a, h) for a in (CAM, Y, X, CORE) for h in hops(a)])
    order = ((CAM, Y, X), (Y, X, CAM), (X, CAM, Y))
    def start(k, stage):
        axis, done = order[k][stage], order[k][:stage]
        first = 9 * k + 3 * stage
        return [send(part(k, done), part(k, done), send_sem.at[first + h - 1], recv_sem.at[first + h - 1], peer(axis, h))
                for h in hops(axis)]

    sent = []
    flying = [start(k, 0) for k in range(3)]
    for stage in range(1, 4):
        for k in range(3):
            for cp in flying[k]:
                cp.wait_recv()
            sent += flying[k]
            if stage < 3:
                flying[k] = start(k, stage)
    half = out_ref.at[:, :, at[CORE]]
    last = send(half, half, send_sem.at[27], recv_sem.at[27], peer(CORE, 1))
    for cp in sent:
        cp.wait_send()
    last.wait()


def gather_rows(local):
    rows = local.shape[0]
    nx, ny, nc, nz = [lax.axis_size(a) for a in (X, Y, CORE, CAM)]
    out = pl.pallas_call(
        gather_body,
        out_shape=jax.ShapeDtypeStruct((nx, ny, nc, nz, rows, 1, 128), F32),
        in_specs=[pl.BlockSpec(memory_space=pltpu.VMEM)],
        out_specs=pl.BlockSpec(memory_space=pltpu.VMEM),
        scratch_shapes=[pltpu.SemaphoreType.DMA((28,)), pltpu.SemaphoreType.DMA((28,))],
        cost_estimate=pl.CostEstimate(flops=20000000000, bytes_accessed=1000000, transcendentals=0),
        compiler_params=pltpu.CompilerParams(collective_id=0, has_side_effects=True, vmem_limit_bytes=8*1024*1024),
        name="gather_rows",
    )(local)
    return out.reshape(nx * ny * nc * nz * rows, 128)


def cost_peers():
    near = [{**peer(Y, i), **peer(CAM, j)} for i in range(4) for j in range(4) if i or j]
    far = [{**peer(X, i), **peer(CORE, j)} for i in range(4) for j in range(2) if i or j]
    return near, far


def cost_body(scale, part_ref, out_ref, buf, send_sem, recv_sem):
    x, y, c, z = [lax.axis_index(a) for a in (X, Y, CORE, CAM)]
    peers = cost_peers()
    greet(peers[0] + peers[1])
    value = part_ref[...]
    slot = 0
    for stage, (me, count) in enumerate(((y * 4 + z, 16), (x * 2 + c, 8))):
        buf[stage, pl.ds(pl.multiple_of(me * 8, 8), 8), :] = value
        own = buf.at[stage, pl.ds(pl.multiple_of(me * 8, 8), 8)]
        copies = []
        for p in peers[stage]:
            copies.append(send(own, own, send_sem.at[slot], recv_sem.at[slot], p))
            slot += 1
        for cp in copies:
            cp.wait()
        value = buf[stage, 0:8, :]
        for k in range(1, count):
            value = value + buf[stage, k * 8:k * 8 + 8, :]
    out_ref[...] = jnp.sum(value, axis=(0, 1), keepdims=True) * scale


def total_cost(part, scale):
    out = pl.pallas_call(
        functools.partial(cost_body, scale),
        out_shape=jax.ShapeDtypeStruct((1, 1), F32),
        in_specs=[pl.BlockSpec(memory_space=pltpu.VMEM)],
        out_specs=pl.BlockSpec(memory_space=pltpu.VMEM),
        scratch_shapes=[pltpu.VMEM((2, 128, 128), F32), pltpu.SemaphoreType.DMA((22,)), pltpu.SemaphoreType.DMA((22,))],
        cost_estimate=pl.CostEstimate(flops=5000000000, bytes_accessed=1000000, transcendentals=0),
        compiler_params=pltpu.CompilerParams(collective_id=1, has_side_effects=True, vmem_limit_bytes=4*1024*1024),
        name="total_cost",
    )(part)
    return out.reshape(())


RT2 = math.sqrt(2.0)


def camera_rows(trial):
    w = [trial[i:i + 1] for i in range(3)]
    half = 0.5 * jnp.sqrt(w[0] * w[0] + w[1] * w[1] + w[2] * w[2])
    zero = half == 0.0
    ratio = (0.5 * RT2) * jnp.where(zero, 1.0, jnp.sin(half) / jnp.where(zero, 1.0, half))
    f = trial[6:7]
    return [ratio * a for a in w] + [RT2 * jnp.cos(half), trial[3:4], trial[4:5], trial[5:6], f, f * trial[7:8], f * trial[8:9]]


def solve_body(red_ref, cam_ref, inc_ref, pts_hbm, grad_hbm, inv_hbm, new_ref, tab_ref, pts, grad, inv, pscr, gscr, iscr,
               far, near, total, local_sem, send_sem, recv_sem):
    cx, cy, cc = [lax.axis_index(a) for a in (X, Y, CORE)]
    z = lax.axis_index(CAM)
    n = lax.axis_size(CAM)
    rows = red_ref.shape[1] // n
    half = rows // 2
    lanes = pl.ds(pl.multiple_of(z * (rows * 128), 128), rows * 128)
    loads = [pltpu.make_async_copy(src.at[:, lanes], dst, local_sem.at[i])
             for i, (src, dst) in enumerate(((pts_hbm, pts), (grad_hbm, grad), (inv_hbm, inv)))]
    for cp in loads:
        cp.start()
    right, left = peer(CAM, 1), peer(CAM, n - 1)
    for i, row in enumerate(camera_rows(cam_ref[...] + inc_ref[...])):
        tab_ref[cx, cy, cc, z, i] = row
    greet([peer(a, h) for a in (CAM, Y, X, CORE) for h in hops(a)])

    def spread_table(axis, part, slot):
        return [send(part, part, send_sem.at[slot + h - 1], recv_sem.at[slot + h - 1], peer(axis, h)) for h in hops(axis)]

    table = spread_table(CAM, tab_ref.at[cx, cy, cc, z], 10)

    def at(k):
        return lax.rem(z + k, n) * rows

    a = send(red_ref.at[:, pl.ds(at(2), half)], far.at[0], send_sem.at[0], recv_sem.at[0], right)
    b = send(red_ref.at[:, pl.ds(at(2) + half, half)], far.at[1], send_sem.at[1], recv_sem.at[1], left)
    c = send(red_ref.at[:, pl.ds(at(1) + half, half)], near.at[0, :, pl.ds(half, half)], send_sem.at[2], recv_sem.at[2], right)
    d = send(red_ref.at[:, pl.ds(at(n - 1), half)], near.at[1, :, pl.ds(0, half)], send_sem.at[3], recv_sem.at[3], left)
    a.wait_recv()
    total[0] = red_ref[:, pl.ds(at(1), half), :] + far[0]
    e = send(total.at[0], near.at[0, :, pl.ds(0, half)], send_sem.at[4], recv_sem.at[4], right)
    b.wait_recv()
    total[1] = red_ref[:, pl.ds(at(n - 1) + half, half), :] + far[1]
    f = send(total.at[1], near.at[1, :, pl.ds(half, half)], send_sem.at[5], recv_sem.at[5], left)
    for cp in table:
        cp.wait()
    table = spread_table(Y, tab_ref.at[cx, cy, cc], 13)
    for cp in loads:
        cp.wait()
    c.wait_recv()
    d.wait_recv()
    e.wait_recv()
    f.wait_recv()

    def group(g, _):
        r8 = pl.ds(pl.multiple_of(g * 8, 8), 8)
        for j in range(8):
            l = pl.ds(pl.multiple_of(g * 1024 + j * 128, 128), 128)
            pscr[pl.ds(j * 8, 3), :] = pts[:, l]
            gscr[pl.ds(j * 8, 3), :] = grad[:, l]
            iscr[pl.ds(j * 16, 9), :] = inv[:, l]
        own = pl.ds(pl.multiple_of(z * rows + g * 8, 8), 8)
        res = [gscr[pl.ds(k, 8, stride=8), :]
               - (red_ref[k, own, :] + near[0, k, r8, :] + near[1, k, r8, :]) for k in range(3)]
        for i in range(3):
            step = (iscr[pl.ds(3 * i, 8, stride=16), :] * res[0] + iscr[pl.ds(3 * i + 1, 8, stride=16), :] * res[1]
                    + iscr[pl.ds(3 * i + 2, 8, stride=16), :] * res[2])
            new_ref[i, own, :] = pscr[pl.ds(i, 8, stride=8), :] + step
        return 0

    def own(part):
        return new_ref.at[:, pl.ds(z * rows + part * half, half)]

    lax.fori_loop(0, half // 8, group, 0)
    g = send(own(0), own(0), send_sem.at[6], recv_sem.at[6], right)
    lax.fori_loop(half // 8, rows // 8, group, 0)
    h = send(own(1), own(1), send_sem.at[7], recv_sem.at[7], left)
    g2 = send(own(1), own(1), send_sem.at[8], recv_sem.at[8], right)
    h2 = send(own(0), own(0), send_sem.at[9], recv_sem.at[9], left)
    for cp in table:
        cp.wait()
    table = spread_table(X, tab_ref.at[cx, :, cc], 16)
    g.wait_recv()
    first = new_ref.at[:, pl.ds(at(n - 1), half)]
    k = send(first, first, send_sem.at[20], recv_sem.at[20], right)
    h.wait_recv()
    second = new_ref.at[:, pl.ds(at(1) + half, half)]
    m = send(second, second, send_sem.at[21], recv_sem.at[21], left)
    for cp in table:
        cp.wait()
    table = spread_table(CORE, tab_ref.at[:, :, cc], 19)
    for cp in (g2, h2, k, m):
        cp.wait_recv()
    for cp in (a, b, c, d, e, f, g, h, g2, h2, k, m):
        cp.wait_send()
    for cp in table:
        cp.wait()


def solve_points(reduced, cameras, increment, points, gradient, inverse):
    rows = reduced.shape[1] // 4
    nx, ny, nc, nz = [lax.axis_size(a) for a in (X, Y, CORE, CAM)]
    hbm = pl.BlockSpec(memory_space=pl.ANY)
    vmem = pl.BlockSpec(memory_space=pltpu.VMEM)
    new, table = pl.pallas_call(
        solve_body,
        out_shape=(jax.ShapeDtypeStruct(reduced.shape, F32), jax.ShapeDtypeStruct((nx, ny, nc, nz, CT, 1, 128), F32)),
        in_specs=[vmem, vmem, vmem, hbm, hbm, hbm],
        out_specs=(vmem, vmem),
        scratch_shapes=[
            pltpu.VMEM((3, rows * 128), F32), pltpu.VMEM((3, rows * 128), F32), pltpu.VMEM((9, rows * 128), F32),
            pltpu.VMEM((64, 128), F32), pltpu.VMEM((64, 128), F32), pltpu.VMEM((128, 128), F32),
            pltpu.VMEM((2, 3, rows // 2, 128), F32), pltpu.VMEM((2, 3, rows, 128), F32),
            pltpu.VMEM((2, 3, rows // 2, 128), F32),
            pltpu.SemaphoreType.DMA((3,)), pltpu.SemaphoreType.DMA((22,)), pltpu.SemaphoreType.DMA((22,)),
        ],
        cost_estimate=pl.CostEstimate(flops=8000000000, bytes_accessed=1000000, transcendentals=0),
        compiler_params=pltpu.CompilerParams(collective_id=2, has_side_effects=True, vmem_limit_bytes=16*1024*1024),
        name="solve_points",
    )(reduced, cameras, increment, points, gradient, inverse)
    return new, table.reshape(nx * ny * nc * nz * CT, 128)


def rows_of(x):
    n = x.shape[1] // 128
    return x.reshape(x.shape[0], n, 128).transpose(1, 0, 2).reshape(n * x.shape[0], 128)


def on_device(cameras, increment, points, gradient, inverse, cj, pj, observed, tb, tp, oc, op, accept):
    oc2 = oc.reshape(-1, 128)
    op2 = op.reshape(-1, 128)
    reduced, kept = reduce_points(gather_rows(increment), cj, pj, oc2, op2, tb, tp, accept.reshape(1), cameras, increment, points.shape[1])
    new, table = solve_points(reduced, cameras, increment, points, gradient, inverse)
    res, accepted, cost = project_points(table, new.reshape(-1, 128), oc2, op2, rows_of(observed), tb, tp, accept.reshape(1), points)
    n = observed.shape[1]
    residual = res.reshape(n // 128, 2, 128).transpose(1, 0, 2).reshape(2, n)
    total = total_cost(cost, 1.0 / (2.0 * n * lax.axis_size(PTS_CAM)))
    return residual, total, accepted, kept


def solution(mesh):
    split = Mesh(mesh.devices.reshape(4, 4, 2, mesh.shape["cam"]), PTS_CAM)
    in_specs = (P(None, PTS_CAM), P(None, PTS_CAM), P(None, PTS), P(None, PTS), P(None, PTS),
                P(None, PTS_CAM), P(None, PTS_CAM), P(None, PTS_CAM),
                P(PTS_CAM), P(PTS_CAM), P(PTS_CAM), P(PTS_CAM), P())
    out_specs = (P(None, PTS_CAM), P(), P(None, PTS), P(None, PTS_CAM))
    return jax.shard_map(on_device, mesh=split, in_specs=in_specs, out_specs=out_specs, check_vma=False)
```

```python
import functools, math
import jax, jax.numpy as jnp
from jax import lax
from jax.experimental import pallas as pl
from jax.experimental.pallas import tpu as pltpu
from jax.sharding import Mesh
from jax.sharding import PartitionSpec as P

CB=128; PB=256; TILE=256
F32=jnp.float32
GROUP=1024
TPG=GROUP//TILE

def lane_gather(table, index):
    return lax.gather(table, index[..., None],
        lax.GatherDimensionNumbers(offset_dims=(), collapsed_slice_dims=(1,), start_index_map=(1,),
            operand_batching_dims=(0,), start_indices_batching_dims=(0,)),
        slice_sizes=(1,1), mode=lax.GatherScatterMode.PROMISE_IN_BOUNDS)

def tile_rows(rows, row_id):
    a,b,c,d = rows
    return jnp.where(row_id<4, jnp.where(row_id<2,a,b), jnp.where(row_id<6,c,d))

def spread(ref, first):
    return ref[pl.ds(first, 8, stride=0), :]

PH=8; PL=32
UN=32

def reduce_body(chunk, blocks_n, tb, tp, word, inc_ref, cj_ref, pj_ref, oc_ref, op_ref, cam_ref, own_ref, out_ref, kept_ref, acc, jscr, pscr, wscr):
    step = 0
    groups = oc_ref.shape[0]//8
    row_id = lax.broadcasted_iota(jnp.int32,(8,128),0)
    if True:
        def zero(i,_):
            acc[pl.ds(pl.multiple_of(i*(PH*8),PH*8),PH*8),:] = jnp.zeros((PH*8,PL),F32)
            return 0
        lax.fori_loop(0, blocks_n, zero, 0, unroll=8)
        wscr[...] = jnp.zeros_like(wscr)
        kept_ref[...] = cam_ref[...] + (word[0] & 1).astype(F32)*own_ref[...]
    def couple(g, slot):
        base = step*(chunk//TILE) + g*TPG
        cams = [tb[base+i]*9 for i in range(TPG)]
        cam = oc_ref[pl.ds(pl.multiple_of(g*8,8),8),:]
        for j in range(8):
            at = pl.ds(pl.multiple_of(g*GROUP+j*128,128),128)
            jscr[slot, j*24:j*24+18,:] = cj_ref[:,at].astype(F32)
            pscr[slot, j*8:j*8+6,:] = pj_ref[:,at].astype(F32)
        first=second=None
        for m in range(9):
            t = tile_rows([spread(inc_ref, c+m) for c in cams], row_id)
            v = lane_gather(t, cam)
            a = jscr[slot, pl.ds(m,8,stride=24),:]*v
            b = jscr[slot, pl.ds(9+m,8,stride=24),:]*v
            first = a if first is None else first+a
            second = b if second is None else second+b
        for n in range(3):
            v = pscr[slot, pl.ds(n,8,stride=8),:]*first + pscr[slot, pl.ds(3+n,8,stride=8),:]*second
            hi = v.astype(jnp.bfloat16).astype(F32)
            wscr[slot, pl.ds(n,8,stride=8),:] = hi
            wscr[slot, pl.ds(3+n,8,stride=8),:] = v-hi
    def scatter(g, slot):
        base = step*(chunk//TILE) + g*TPG
        for t in range(TPG):
            lhs=[]; rhs=[]
            for h in range(2):
                s=2*t+h
                w = wscr[slot, s*8:s*8+8,:]
                ids = op_ref[pl.ds(g*8+s,8,stride=0),:]
                hi = lax.shift_right_logical(ids,PL.bit_length()-1)
                lo = ids & (PL-1)
                lhs.append(jnp.concatenate([jnp.where(hi==k,w,0.0) for k in range(PH)],axis=0).astype(jnp.bfloat16))
                rhs.append(jnp.concatenate([jnp.where(lo-8*k==row_id,1.0,0.0) for k in range(PL//8)],axis=0).astype(jnp.bfloat16))
            L=jnp.concatenate(lhs,axis=1); R=jnp.concatenate(rhs,axis=1)
            r = lax.dot_general(L,R,(((1,),(1,)),((),())),preferred_element_type=F32)
            at = pl.ds(pl.multiple_of(tp[base+t]*(PH*8),PH*8),PH*8)
            acc[at,:] += r
    def body(i,_):
        for u in range(UN): couple(i*UN+u, u)
        for u in range(UN): scatter(i*UN+u, u)
        return 0
    lax.fori_loop(0, groups//UN, body, 0)
    if True:
        def flush(i,_):
            for h in range(2):
                n = 128//PL
                x = jnp.concatenate([acc[pl.ds(pl.multiple_of(i*(PH*8)+(h*n+k)*8,8),8),:] for k in range(n)],axis=1)
                s = x[0:3,:]+x[3:6,:]
                for n in range(3):
                    out_ref[n, pl.ds(2*i+h,1),:] = s[n:n+1,:]
            return 0
        lax.fori_loop(0, blocks_n, flush, 0, unroll=32)

def reduce_points(inc, cj, pj, oc, op, tb, tp, word, cameras, increment, npts, chunk=16384):
    n=cj.shape[1]
    blocks_n=npts//PB
    return pl.pallas_call(
        functools.partial(reduce_body, chunk, blocks_n),
        out_shape=(jax.ShapeDtypeStruct((3,npts//128,128),F32), jax.ShapeDtypeStruct((9,128),F32)),
        in_specs=[pl.BlockSpec(memory_space=pltpu.SMEM)]*3+[pl.BlockSpec(memory_space=pltpu.VMEM)]*7,
        out_specs=(pl.BlockSpec(memory_space=pltpu.VMEM), pl.BlockSpec(memory_space=pltpu.VMEM)),
            scratch_shapes=[pltpu.VMEM((blocks_n*PH*8,PL),F32), pltpu.VMEM((UN,192,128),F32), pltpu.VMEM((UN,64,128),F32), pltpu.VMEM((UN,64,128),F32)],
        cost_estimate=pl.CostEstimate(flops=10000000000, bytes_accessed=1000000, transcendentals=0),
        compiler_params=pltpu.CompilerParams(vmem_limit_bytes=28*1024*1024),
        name="reduce_points",
    )(tb,tp,word,inc,cj,pj,oc,op,cameras,increment)

CT=10
TURN=16

def project_body(tb, tp, word, cam_ref, pts_ref, oc_ref, op_ref, ob_ref, old_ref, res_hbm, acc_hbm, cost_ref, res_ref, acc_ref, sem):
    turns=oc_ref.shape[0]//(8*TURN)
    spans=old_ref.shape[1]//(128*turns)
    row_id=lax.broadcasted_iota(jnp.int32,(8,128),0)
    taken=jnp.broadcast_to(word[0]&1,(3,128))==1
    def one(g):
        base=g*TPG
        cams=[tb[base+i]*CT for i in range(TPG)]
        pts=[tp[base+i]*2 for i in range(TPG)]
        at8=pl.ds(pl.multiple_of(g*8,8),8)
        cam=oc_ref[at8,:]; pid=op_ref[at8,:]
        half=pts_ref.shape[0]//3
        upper=pid>=128; plow=pid&127
        def look(r): return lane_gather(tile_rows([spread(cam_ref,c+r) for c in cams],row_id),cam)
        def lookp(r):
            a=lane_gather(tile_rows([spread(pts_ref,p+r*half) for p in pts],row_id),plow)
            b=lane_gather(tile_rows([spread(pts_ref,p+r*half+1) for p in pts],row_id),plow)
            return jnp.where(upper,b,a)
        x,y,z=lookp(0),lookp(1),lookp(2)
        vx,vy,vz,r,t0,t1,t2,f0,f1,f2=[look(i) for i in range(CT)]
        ax=vy*z-vz*y; ay=vz*x-vx*z; az=vx*y-vy*x
        px=x+r*ax+(vy*az-vz*ay)+t0
        py=y+r*ay+(vz*ax-vx*az)+t1
        pz=z+r*az+(vx*ay-vy*ax)+t2
        inv=1.0/jnp.maximum(-pz,1.0)
        u=px*inv; v=py*inv
        q=u*u+v*v
        fac=f0+q*(f1+q*f2)
        o0=pl.ds(g*16,8,stride=2); o1=pl.ds(g*16+1,8,stride=2)
        ru=fac*u-ob_ref[o0,:]; rv=fac*v-ob_ref[o1,:]
        res_ref[o0,:]=ru; res_ref[o1,:]=rv
        return ru*ru+rv*rv
    def out(i):
        rows=pl.ds(pl.multiple_of(i*(TURN*16),TURN*16),TURN*16)
        lanes=pl.ds(pl.multiple_of(i*(spans*128),spans*128),spans*128)
        return (pltpu.make_async_copy(res_ref.at[rows],res_hbm.at[rows],sem.at[0,i]),
                pltpu.make_async_copy(acc_ref.at[:,lanes],acc_hbm.at[:,lanes],sem.at[1,i]))
    def body(i,c):
        for u in range(TURN): c=c+one(i*TURN+u)
        for j in range(spans):
            row=i*spans+j
            lanes=pl.ds(pl.multiple_of(row*128,128),128)
            new=jnp.concatenate([pts_ref[pl.ds(row+k*(spans*turns),1),:] for k in range(3)],axis=0)
            acc_ref[:,lanes]=jnp.where(taken,new,old_ref[:,lanes])
        for cp in out(i): cp.start()
        return c
    cost_ref[...]=lax.fori_loop(0,turns,body,jnp.zeros((8,128),F32))
    def finish(i,_):
        for cp in out(i): cp.wait()
        return 0
    lax.fori_loop(0,turns,finish,0)

def project_points(cam, pts, oc, op, ob, tb, tp, word, old):
    n=oc.shape[0]*128
    turns=n//(GROUP*TURN)
    smem=pl.BlockSpec(memory_space=pltpu.SMEM)
    vmem=pl.BlockSpec(memory_space=pltpu.VMEM)
    hbm=pl.BlockSpec(memory_space=pl.ANY)
    return pl.pallas_call(
        project_body,
        out_shape=(jax.ShapeDtypeStruct((n//64,128),F32), jax.ShapeDtypeStruct(old.shape,F32), jax.ShapeDtypeStruct((8,128),F32)),
        in_specs=[smem]*3+[vmem]*6,
        out_specs=(hbm,hbm,vmem),
        scratch_shapes=[pltpu.VMEM((n//64,128),F32), pltpu.VMEM(old.shape,F32), pltpu.SemaphoreType.DMA((2,turns))],
        cost_estimate=pl.CostEstimate(flops=5000000000, bytes_accessed=1000000, transcendentals=0),
        compiler_params=pltpu.CompilerParams(vmem_limit_bytes=20*1024*1024),
        name="project_points",
    )(tb,tp,word,cam,pts,oc,op,ob,old)


MESH = pl.DeviceIdType.MESH
X, Y, CORE, CAM = "pts_0", "pts_1", "pts_2", "cam"
PTS = (X, Y, CORE)
PTS_CAM = PTS + (CAM,)


def peer(axis, hop):
    n = lax.axis_size(axis)
    return {axis: lax.rem(lax.axis_index(axis) + hop, n)}


def greet(peers):
    barrier = pltpu.get_barrier_semaphore()
    for p in peers:
        pl.semaphore_signal(barrier, inc=1, device_id=p, device_id_type=MESH)
    pl.semaphore_wait(barrier, len(peers))


def hops(axis):
    return range(1, lax.axis_size(axis))


def send(src, dst, send_sem, recv_sem, to):
    copy = pltpu.make_async_remote_copy(src, dst, send_sem, recv_sem, device_id=to, device_id_type=MESH)
    copy.start()
    return copy


def gather_body(local_ref, out_ref, send_sem, recv_sem):
    at = {a: lax.axis_index(a) for a in (X, Y, CORE, CAM)}

    def part(k, whole):
        i = [slice(None) if a in whole else at[a] for a in (X, Y, CORE, CAM)]
        return out_ref.at[(*i, pl.ds(3 * k, 3))]

    for i in range(9):
        out_ref[at[X], at[Y], at[CORE], at[CAM], i] = local_ref[i:i + 1, :]
    greet([peer(a, h) for a in (CAM, Y, X, CORE) for h in hops(a)])
    order = ((CAM, Y, X), (Y, X, CAM), (X, CAM, Y))
    def start(k, stage):
        axis, done = order[k][stage], order[k][:stage]
        first = 9 * k + 3 * stage
        return [send(part(k, done), part(k, done), send_sem.at[first + h - 1], recv_sem.at[first + h - 1], peer(axis, h))
                for h in hops(axis)]

    sent = []
    flying = [start(k, 0) for k in range(3)]
    for stage in range(1, 4):
        for k in range(3):
            for cp in flying[k]:
                cp.wait_recv()
            sent += flying[k]
            if stage < 3:
                flying[k] = start(k, stage)
    half = out_ref.at[:, :, at[CORE]]
    last = send(half, half, send_sem.at[27], recv_sem.at[27], peer(CORE, 1))
    for cp in sent:
        cp.wait_send()
    last.wait()


def gather_rows(local):
    rows = local.shape[0]
    nx, ny, nc, nz = [lax.axis_size(a) for a in (X, Y, CORE, CAM)]
    out = pl.pallas_call(
        gather_body,
        out_shape=jax.ShapeDtypeStruct((nx, ny, nc, nz, rows, 1, 128), F32),
        in_specs=[pl.BlockSpec(memory_space=pltpu.VMEM)],
        out_specs=pl.BlockSpec(memory_space=pltpu.VMEM),
        scratch_shapes=[pltpu.SemaphoreType.DMA((28,)), pltpu.SemaphoreType.DMA((28,))],
        cost_estimate=pl.CostEstimate(flops=20000000000, bytes_accessed=1000000, transcendentals=0),
        compiler_params=pltpu.CompilerParams(collective_id=0, has_side_effects=True, vmem_limit_bytes=8*1024*1024),
        name="gather_rows",
    )(local)
    return out.reshape(nx * ny * nc * nz * rows, 128)


def cost_peers():
    near = [{**peer(Y, i), **peer(CAM, j)} for i in range(4) for j in range(4) if i or j]
    far = [{**peer(X, i), **peer(CORE, j)} for i in range(4) for j in range(2) if i or j]
    return near, far


def cost_body(scale, part_ref, out_ref, buf, send_sem, recv_sem):
    x, y, c, z = [lax.axis_index(a) for a in (X, Y, CORE, CAM)]
    peers = cost_peers()
    greet(peers[0] + peers[1])
    value = jnp.sum(part_ref[...], axis=0, keepdims=True)
    slot = 0
    sent = []
    for stage, (me, count) in enumerate(((y * 4 + z, 16), (x * 2 + c, 8))):
        buf[stage, me] = value
        own = buf.at[stage, me]
        copies = []
        for p in peers[stage]:
            copies.append(send(own, own, send_sem.at[slot], recv_sem.at[slot], p))
            slot += 1
        for cp in copies:
            cp.wait_recv()
        sent += copies
        value = buf[stage, 0]
        for k in range(1, count):
            value = value + buf[stage, k]
    out_ref[...] = jnp.sum(value, axis=(0, 1), keepdims=True) * scale
    for cp in sent:
        cp.wait_send()


def total_cost(part, scale):
    out = pl.pallas_call(
        functools.partial(cost_body, scale),
        out_shape=jax.ShapeDtypeStruct((1, 1), F32),
        in_specs=[pl.BlockSpec(memory_space=pltpu.VMEM)],
        out_specs=pl.BlockSpec(memory_space=pltpu.VMEM),
        scratch_shapes=[pltpu.VMEM((2, 16, 1, 128), F32), pltpu.SemaphoreType.DMA((22,)), pltpu.SemaphoreType.DMA((22,))],
        cost_estimate=pl.CostEstimate(flops=5000000000, bytes_accessed=1000000, transcendentals=0),
        compiler_params=pltpu.CompilerParams(collective_id=1, has_side_effects=True, vmem_limit_bytes=4*1024*1024),
        name="total_cost",
    )(part)
    return out.reshape(())


RT2 = math.sqrt(2.0)


def camera_rows(trial):
    w = [trial[i:i + 1] for i in range(3)]
    half = 0.5 * jnp.sqrt(w[0] * w[0] + w[1] * w[1] + w[2] * w[2])
    zero = half == 0.0
    ratio = (0.5 * RT2) * jnp.where(zero, 1.0, jnp.sin(half) / jnp.where(zero, 1.0, half))
    f = trial[6:7]
    return [ratio * a for a in w] + [RT2 * jnp.cos(half), trial[3:4], trial[4:5], trial[5:6], f, f * trial[7:8], f * trial[8:9]]


def solve_body(red_ref, cam_ref, inc_ref, pts_hbm, grad_hbm, inv_hbm, new_ref, tab_ref, pts, grad, inv, pscr, gscr, iscr,
               far, near, total, local_sem, send_sem, recv_sem):
    cx, cy, cc = [lax.axis_index(a) for a in (X, Y, CORE)]
    z = lax.axis_index(CAM)
    n = lax.axis_size(CAM)
    rows = red_ref.shape[1] // n
    half = rows // 2
    lanes = pl.ds(pl.multiple_of(z * (rows * 128), 128), rows * 128)
    loads = [pltpu.make_async_copy(src.at[:, lanes], dst, local_sem.at[i])
             for i, (src, dst) in enumerate(((pts_hbm, pts), (grad_hbm, grad), (inv_hbm, inv)))]
    for cp in loads:
        cp.start()
    right, left = peer(CAM, 1), peer(CAM, n - 1)
    for i, row in enumerate(camera_rows(cam_ref[...] + inc_ref[...])):
        tab_ref[cx, cy, cc, z, i] = row
    greet([peer(a, h) for a in (CAM, Y, X, CORE) for h in hops(a)])

    def spread_table(axis, part, slot):
        return [send(part, part, send_sem.at[slot + h - 1], recv_sem.at[slot + h - 1], peer(axis, h)) for h in hops(axis)]

    table = spread_table(CAM, tab_ref.at[cx, cy, cc, z], 10)

    def at(k):
        return lax.rem(z + k, n) * rows

    a = send(red_ref.at[:, pl.ds(at(2), half)], far.at[0], send_sem.at[0], recv_sem.at[0], right)
    b = send(red_ref.at[:, pl.ds(at(2) + half, half)], far.at[1], send_sem.at[1], recv_sem.at[1], left)
    c = send(red_ref.at[:, pl.ds(at(1) + half, half)], near.at[0, :, pl.ds(half, half)], send_sem.at[2], recv_sem.at[2], right)
    d = send(red_ref.at[:, pl.ds(at(n - 1), half)], near.at[1, :, pl.ds(0, half)], send_sem.at[3], recv_sem.at[3], left)
    a.wait_recv()
    total[0] = red_ref[:, pl.ds(at(1), half), :] + far[0]
    e = send(total.at[0], near.at[0, :, pl.ds(0, half)], send_sem.at[4], recv_sem.at[4], right)
    b.wait_recv()
    total[1] = red_ref[:, pl.ds(at(n - 1) + half, half), :] + far[1]
    f = send(total.at[1], near.at[1, :, pl.ds(half, half)], send_sem.at[5], recv_sem.at[5], left)
    for cp in table:
        cp.wait()
    table = spread_table(Y, tab_ref.at[cx, cy, cc], 13)
    for cp in loads:
        cp.wait()
    c.wait_recv()
    d.wait_recv()
    e.wait_recv()
    f.wait_recv()

    def group(g, _):
        r8 = pl.ds(pl.multiple_of(g * 8, 8), 8)
        for j in range(8):
            l = pl.ds(pl.multiple_of(g * 1024 + j * 128, 128), 128)
            pscr[pl.ds(j * 8, 3), :] = pts[:, l]
            gscr[pl.ds(j * 8, 3), :] = grad[:, l]
            iscr[pl.ds(j * 16, 9), :] = inv[:, l]
        own = pl.ds(pl.multiple_of(z * rows + g * 8, 8), 8)
        res = [gscr[pl.ds(k, 8, stride=8), :]
               - (red_ref[k, own, :] + near[0, k, r8, :] + near[1, k, r8, :]) for k in range(3)]
        for i in range(3):
            step = (iscr[pl.ds(3 * i, 8, stride=16), :] * res[0] + iscr[pl.ds(3 * i + 1, 8, stride=16), :] * res[1]
                    + iscr[pl.ds(3 * i + 2, 8, stride=16), :] * res[2])
            new_ref[i, own, :] = pscr[pl.ds(i, 8, stride=8), :] + step
        return 0

    def own(part):
        return new_ref.at[:, pl.ds(z * rows + part * half, half)]

    lax.fori_loop(0, half // 8, group, 0)
    g = send(own(0), own(0), send_sem.at[6], recv_sem.at[6], right)
    lax.fori_loop(half // 8, rows // 8, group, 0)
    h = send(own(1), own(1), send_sem.at[7], recv_sem.at[7], left)
    g2 = send(own(1), own(1), send_sem.at[8], recv_sem.at[8], right)
    h2 = send(own(0), own(0), send_sem.at[9], recv_sem.at[9], left)
    for cp in table:
        cp.wait()
    table = spread_table(X, tab_ref.at[cx, :, cc], 16)
    g.wait_recv()
    first = new_ref.at[:, pl.ds(at(n - 1), half)]
    k = send(first, first, send_sem.at[20], recv_sem.at[20], right)
    h.wait_recv()
    second = new_ref.at[:, pl.ds(at(1) + half, half)]
    m = send(second, second, send_sem.at[21], recv_sem.at[21], left)
    for cp in table:
        cp.wait()
    table = spread_table(CORE, tab_ref.at[:, :, cc], 19)
    for cp in (g2, h2, k, m):
        cp.wait_recv()
    for cp in (a, b, c, d, e, f, g, h, g2, h2, k, m):
        cp.wait_send()
    for cp in table:
        cp.wait()


def solve_points(reduced, cameras, increment, points, gradient, inverse):
    rows = reduced.shape[1] // 4
    nx, ny, nc, nz = [lax.axis_size(a) for a in (X, Y, CORE, CAM)]
    hbm = pl.BlockSpec(memory_space=pl.ANY)
    vmem = pl.BlockSpec(memory_space=pltpu.VMEM)
    new, table = pl.pallas_call(
        solve_body,
        out_shape=(jax.ShapeDtypeStruct(reduced.shape, F32), jax.ShapeDtypeStruct((nx, ny, nc, nz, CT, 1, 128), F32)),
        in_specs=[vmem, vmem, vmem, hbm, hbm, hbm],
        out_specs=(vmem, vmem),
        scratch_shapes=[
            pltpu.VMEM((3, rows * 128), F32), pltpu.VMEM((3, rows * 128), F32), pltpu.VMEM((9, rows * 128), F32),
            pltpu.VMEM((64, 128), F32), pltpu.VMEM((64, 128), F32), pltpu.VMEM((128, 128), F32),
            pltpu.VMEM((2, 3, rows // 2, 128), F32), pltpu.VMEM((2, 3, rows, 128), F32),
            pltpu.VMEM((2, 3, rows // 2, 128), F32),
            pltpu.SemaphoreType.DMA((3,)), pltpu.SemaphoreType.DMA((22,)), pltpu.SemaphoreType.DMA((22,)),
        ],
        cost_estimate=pl.CostEstimate(flops=8000000000, bytes_accessed=1000000, transcendentals=0),
        compiler_params=pltpu.CompilerParams(collective_id=2, has_side_effects=True, vmem_limit_bytes=16*1024*1024),
        name="solve_points",
    )(reduced, cameras, increment, points, gradient, inverse)
    return new, table.reshape(nx * ny * nc * nz * CT, 128)


def rows_of(x):
    n = x.shape[1] // 128
    return x.reshape(x.shape[0], n, 128).transpose(1, 0, 2).reshape(n * x.shape[0], 128)


def on_device(cameras, increment, points, gradient, inverse, cj, pj, observed, tb, tp, oc, op, accept):
    oc2 = oc.reshape(-1, 128)
    op2 = op.reshape(-1, 128)
    reduced, kept = reduce_points(gather_rows(increment), cj, pj, oc2, op2, tb, tp, accept.reshape(1), cameras, increment, points.shape[1])
    new, table = solve_points(reduced, cameras, increment, points, gradient, inverse)
    res, accepted, cost = project_points(table, new.reshape(-1, 128), oc2, op2, rows_of(observed), tb, tp, accept.reshape(1), points)
    n = observed.shape[1]
    residual = res.reshape(n // 128, 2, 128).transpose(1, 0, 2).reshape(2, n)
    total = total_cost(cost, 1.0 / (2.0 * n * lax.axis_size(PTS_CAM)))
    return residual, total, accepted, kept


def solution(mesh):
    split = Mesh(mesh.devices.reshape(4, 4, 2, mesh.shape["cam"]), PTS_CAM)
    in_specs = (P(None, PTS_CAM), P(None, PTS_CAM), P(None, PTS), P(None, PTS), P(None, PTS),
                P(None, PTS_CAM), P(None, PTS_CAM), P(None, PTS_CAM),
                P(PTS_CAM), P(PTS_CAM), P(PTS_CAM), P(PTS_CAM), P())
    out_specs = (P(None, PTS_CAM), P(), P(None, PTS), P(None, PTS_CAM))
    return jax.shard_map(on_device, mesh=split, in_specs=in_specs, out_specs=out_specs, check_vma=False)
```
